256 devices in a mesh: dom: 256 (over y, z, x, core).
Axes of the slice: x: 4, y: 4, z: 8, core: 2. Of those that a mesh axis runs over, the one named last changes fastest.
Arguments:
- rhs: float32 [1024, 12, 512], P('dom'), may hold values from -18 to 18
- stiffness: float32 [512, 512], replicated, may hold values from -0.25 to 0.25
- vol_jac: float32 [1024, 12, 12], P('dom'), may hold values from -0.9 to 0.9
- face_jac: float32 [1024, 6, 12, 12], P('dom'), may hold values from -1.5 to 1.5
- block_inv: float32 [1024, 12, 12, 512], P('dom'), as said below
- face_owner: int32 [1024, 6], P('dom'), may hold values from -1 to 255, as said below
- face_elem: int32 [1024, 6], P('dom'), may hold values from 0 to 3
- face_side: int32 [1024, 6], P('dom'), may hold values from 0 to 5
- face_turn: int32 [1024, 6], P('dom'), may hold values from 0 to 7
Outputs:
- correction: float32 [1024, 12, 512], P('dom')
The draws below stay inside these ranges and needn't reach their ends.
Inputs may be any that keep to these rules, and one draw needn't show every extreme that they name: `face_owner`: -1 marks a face with no neighbour; any other value is the element's own partition or one next to it along the axis; of the faces of one partition exactly 8 name the partition below and exactly 8 the partition above, where that partition exists. Each block_inv[e, :, :, m] is a full 12 x 12 matrix.
All inputs are finite; a program needn't handle non-finite values.
Results may differ from the reference program's by a relative error of at most 0.0001.
Values sent between devices are 32-bit elements; how exact they have to be, the bound alone decides.
No kernel may reach another device: no remote copies, remote signals or barrier semaphores. Data moves between devices by JAX's collectives and lax.ppermute only.
A program may use at most 64 MiB of HBM per device.

```python
import jax
import jax.numpy as jnp
from jax import lax

VARS = 12
QF = 8
QC = 4
E_DEV = 4
MODES = 512
ELEMS = 1024


def draw_block_inv(key, part):
    first_key, second_key = jax.random.split(jax.random.fold_in(key, 11))
    diagonal = jnp.exp(jax.random.uniform(first_key, (ELEMS, VARS, MODES), jnp.float32, jnp.log(0.2), jnp.log(0.5)))
    spread = 0.05 * jax.random.normal(second_key, (ELEMS, VARS, VARS, MODES), jnp.float32)
    identity = (jnp.arange(VARS)[:, None] == jnp.arange(VARS)[None, :]).astype(jnp.float32)[:, :, None]
    return spread * (1.0 - identity) + identity * diagonal[:, :, None, :]


def draw_face_owner(key, part):
    first_key, second_key = jax.random.split(jax.random.fold_in(key, 23))
    partitions = ELEMS // E_DEV
    face_count = 6 * E_DEV
    part_keys = jax.random.split(first_key, partitions)
    orders = jax.vmap(lambda single: jax.random.permutation(single, face_count))(part_keys)
    offset = jnp.where(orders < 2 * E_DEV, -1, jnp.where(orders < 4 * E_DEV, 1, 0)).astype(jnp.int32).reshape(ELEMS, 6)
    dropped = (jax.random.randint(second_key, (ELEMS, 6), 0, 8, jnp.int32) == 0) & (offset == 0)
    home_part = (jnp.arange(ELEMS, dtype=jnp.int32) // E_DEV)[:, None]
    owner = home_part + offset
    outside = dropped | (owner < 0) | (owner >= partitions)
    return jnp.where(outside, -1, owner).astype(jnp.int32)


def touch_ends(result, key, low, largest):
    longest = result.shape.index(max(result.shape))
    spots = []
    for shift in (0, 1):
        where = [jax.random.randint(jax.random.fold_in(key, axis), (), 0, length) for axis, length in enumerate(result.shape)]
        where[longest] = (where[longest] + shift) % result.shape[longest]
        spots.append(tuple(where))
    return result.at[spots[0]].set(low).at[spots[1]].set(largest)


def block_scale(key, shape, cuts, least, top_value):
    factor_of = 1.0
    for axis_at, blocks in cuts:
        steps = jax.random.uniform(jax.random.fold_in(jax.random.fold_in(key, 6), axis_at), (blocks,), jnp.float32, least / len(cuts), top_value / len(cuts))
        factor_of = factor_of * jnp.repeat(jnp.exp(steps), shape[axis_at] // blocks).reshape((-1,) + (1,) * (len(shape) - 1 - axis_at))
    return factor_of


def scatter_about(own_key, extent, width, most, cuts=(), kind=jnp.bfloat16):
    result = width * jax.random.normal(own_key, extent, jnp.float32)
    if cuts:
        result = result * block_scale(own_key, extent, cuts, -0.22, 0.18)
    return jnp.clip(result, -most, most).astype(kind)


def setup_inputs(seed: int = 0) -> dict:
    key_list = jax.random.split(jax.random.key(seed), 10)
    rhs = scatter_about(key_list[0], (ELEMS, VARS, MODES), 3.0, 18.0, ((0, 256),), jnp.float32)
    stiffness = scatter_about(key_list[1], (MODES, MODES), MODES ** -0.5, 0.25, (), jnp.float32)
    vol_jac = scatter_about(key_list[2], (ELEMS, VARS, VARS), 0.15, 0.9, ((0, 256),), jnp.float32)
    face_jac = scatter_about(key_list[3], (ELEMS, 6, VARS, VARS), 0.25, 1.5, ((0, 256),), jnp.float32)
    block_inv = draw_block_inv(jax.random.fold_in(key_list[9], 71), 0)
    face_owner = draw_face_owner(jax.random.fold_in(key_list[9], 71), 0)
    face_elem = touch_ends(jax.random.randint(key_list[6], (ELEMS, 6), 0, E_DEV), jax.random.fold_in(key_list[6], 1), 0, E_DEV - 1).astype(jnp.int32)
    face_side = touch_ends(jax.random.randint(key_list[7], (ELEMS, 6), 0, 6), jax.random.fold_in(key_list[7], 1), 0, 5).astype(jnp.int32)
    face_turn = touch_ends(jax.random.randint(key_list[8], (ELEMS, 6), 0, 8), jax.random.fold_in(key_list[8], 1), 0, 7).astype(jnp.int32)
    return {"rhs": rhs, "stiffness": stiffness, "vol_jac": vol_jac, "face_jac": face_jac, "block_inv": block_inv, "face_owner": face_owner, "face_elem": face_elem, "face_side": face_side, "face_turn": face_turn}


PRECISE = lax.Precision.HIGHEST
SIGMA = 2.0
OMEGA = 0.7


def alternate(degree_count):
    return jnp.where(jnp.arange(degree_count) % 2 == 1, -1.0, 1.0).astype(jnp.float32)


def orient_faces(values, turning):
    degree_count = values.shape[-1]
    flipped = jnp.where((turning % 2 == 1)[:, None, None, None], jnp.swapaxes(values, -1, -2), values)
    signs = alternate(degree_count)
    first_sign = jnp.where(((turning // 2) % 2 == 1)[:, None], signs[None, :], 1.0)
    second_sign = jnp.where(((turning // 4) % 2 == 1)[:, None], signs[None, :], 1.0)
    return flipped * first_sign[:, None, :, None] * second_sign[:, None, None, :]


def apply_operator(iterate, vol_jac, face_jac, kernel, face_owner, face_elem, face_side, face_turn, degree_count):
    elements, variables, mode_count = iterate.shape
    cubed = iterate.reshape(elements, variables, degree_count, degree_count, degree_count)
    einsum_forms = ("evijk,i->evjk", "evijk,j->evik", "evijk,k->evij")
    degree = jnp.arange(degree_count).astype(jnp.float32)
    weight_list = []
    traces = []
    for face_id in range(6):
        if face_id % 2 == 0:
            weight_vec = alternate(degree_count)
        else:
            weight_vec = jnp.ones((degree_count,), jnp.float32)
        weight_list.append(weight_vec)
        traces.append(jnp.einsum(einsum_forms[face_id // 2], cubed, weight_vec, precision=PRECISE))
    trace_all = jnp.stack(traces, axis=1)
    present = face_owner >= 0
    slot_ids = jnp.clip(face_owner * (E_DEV * 6) + face_elem * 6 + face_side, 0, elements * 6 - 1).astype(jnp.int32)
    outside = trace_all.reshape(elements * 6, variables, degree_count, degree_count)[slot_ids.reshape(-1)]
    outside = orient_faces(outside, face_turn.reshape(-1)).reshape(elements, 6, variables, degree_count, degree_count)
    outside = outside * present.astype(jnp.float32)[:, :, None, None, None]
    jumps = jnp.einsum("efvw,efwab->efvab", face_jac, trace_all - outside, precision=PRECISE)
    lifted = jnp.zeros(cubed.shape, jnp.float32)
    for face_id in range(6):
        lift_coef = (2.0 * degree + 1.0) / 16.0 * weight_list[face_id]
        sheet_vals = jumps[:, face_id]
        normal_axis = face_id // 2
        if normal_axis == 0:
            lifted = lifted + sheet_vals[:, :, None, :, :] * lift_coef[:, None, None]
        elif normal_axis == 1:
            lifted = lifted + sheet_vals[:, :, :, None, :] * lift_coef[:, None]
        else:
            lifted = lifted + sheet_vals[:, :, :, :, None] * lift_coef
    blended = jnp.dot(iterate.reshape(elements * variables, mode_count), kernel, precision=PRECISE)
    volume = jnp.einsum("evw,ewm->evm", vol_jac, blended.reshape(elements, variables, mode_count), precision=PRECISE)
    return SIGMA * iterate + volume + lifted.reshape(elements, variables, mode_count)


def shrink(values):
    leading = values.shape[:-1]
    cubed = values.reshape(leading + (QF, QF, QF))[..., :QC, :QC, :QC]
    return cubed.reshape(leading + (QC * QC * QC,))


def widen(values):
    leading = values.shape[:-1]
    cubed = values.reshape(leading + (QC, QC, QC))
    padding = tuple((0, 0) for level in leading) + ((0, QF - QC), (0, QF - QC), (0, QF - QC))
    return jnp.pad(cubed, padding).reshape(leading + (QF * QF * QF,))


def precondition(inverse, residual):
    return jnp.einsum("evwm,ewm->evm", inverse, residual, precision=PRECISE)


def reference(rhs, stiffness, vol_jac, face_jac, block_inv, face_owner, face_elem, face_side, face_turn):
    def fine_apply(iterate):
        return apply_operator(iterate, vol_jac, face_jac, stiffness, face_owner, face_elem, face_side, face_turn, QF)

    coarse_mat = shrink(shrink(stiffness).T).T

    def coarse_apply(iterate):
        return apply_operator(iterate, vol_jac, face_jac, coarse_mat, face_owner, face_elem, face_side, face_turn, QC)

    iterate = OMEGA * precondition(block_inv, rhs)
    iterate = iterate + OMEGA * precondition(block_inv, rhs - fine_apply(iterate))
    coarse_rhs = shrink(rhs - fine_apply(iterate))
    coarse_inv = shrink(block_inv)
    sweep_one = OMEGA * precondition(coarse_inv, coarse_rhs)
    sweep_two = sweep_one + OMEGA * precondition(coarse_inv, coarse_rhs - coarse_apply(sweep_one))
    iterate = iterate + widen(sweep_two)
    for sweep in range(2):
        iterate = iterate + OMEGA * precondition(block_inv, rhs - fine_apply(iterate))
    return iterate
```

```python
import jax
import jax.numpy as jnp
import numpy as np
from jax import lax
from jax.experimental import pallas as pl
from jax.experimental.pallas import tpu as pltpu
from jax.sharding import PartitionSpec as P


QF = 8
QC = 4
VARS = 12
SIGMA = 2.0
OMEGA = 0.7
F32 = jnp.float32
BF16 = jnp.bfloat16
VMEM = pltpu.VMEM


def trace_matrix():
    matrix = np.zeros((512, 384), np.float32)
    for i in range(QF):
        for j in range(QF):
            for k in range(QF):
                mode = (i * QF + j) * QF + k
                triple = (i, j, k)
                for face in range(6):
                    normal = triple[face // 2]
                    a, b = [triple[place] for place in range(3) if place != face // 2]
                    matrix[mode, face * 64 + a * 8 + b] = (-1.0) ** normal if face % 2 == 0 else 1.0
    return matrix


def lift_matrix():
    degrees = np.stack(np.meshgrid(*[np.arange(QF)] * 3, indexing="ij"), -1).reshape(512, 3)
    scale = np.stack([(2.0 * degrees[:, face // 2] + 1.0) / 16.0 for face in range(6)], -1)
    return (trace_matrix().reshape(512, 6, 64) * scale[:, :, None]).reshape(512, 384).T


def rows8():
    return lax.broadcasted_iota(jnp.int32, (8, 128), 0)


def lanes8():
    return lax.broadcasted_iota(jnp.int32, (8, 128), 1)


def half_swap(tile):
    return pltpu.roll(tile, 4, axis=0)


def pair_turn(first, second, low):
    return jnp.where(low, first, half_swap(second)), jnp.where(low, half_swap(first), second)


def prepare_body(me_ref, owner_ref, elem_ref, side_ref, turn_ref, vj_ref, fj_ref, stiff_ref,
                 start_ref, idx_ref, sign_ref, vjc_ref, fjc_ref, khi_ref, klo_ref):
    me = me_ref[0]
    rows = rows8()
    lane = lanes8()
    low = rows < 4
    element = rows & 3
    a = (lane >> 3) & 7
    b = lane & 7
    signs = []
    for face in range(6):
        swap = jnp.zeros((8, 128), jnp.int32)
        parity = jnp.zeros((8, 128), jnp.int32)
        turns = jnp.zeros((8, 128), jnp.int32)
        present = jnp.zeros((8, 128), jnp.int32)
        for e in range(4):
            owner = owner_ref[e, face]
            side = side_ref[e, face]
            block = jnp.where(owner == me, 0, jnp.where(owner == (me ^ 1), 1, 2))
            block = jnp.where(owner < 0, 0, block)
            start_ref[face * 4 + e] = block * 144 + (side >> 1) * 48 + elem_ref[e, face]
            here = element == e
            turns = jnp.where(here, turn_ref[e, face], turns)
            parity = jnp.where(here, side & 1, parity)
            present = jnp.where(here, jnp.where(owner >= 0, 1, 0), present)
        swap = turns & 1
        idx_ref[face] = parity * 64 + jnp.where(swap == 1, b * 8 + a, a * 8 + b)
        flips = (((turns >> 1) & a) + ((turns >> 2) & b)) & 1
        signs.append((present * (1 - 2 * flips)).astype(F32))
    for f2 in range(3):
        sign_ref[f2] = jnp.where(lane < 64, signs[2 * f2], signs[2 * f2 + 1])
    for vp in range(6):
        block = vj_ref[vp]
        for w in range(VARS):
            spread = jnp.broadcast_to(block[:, w : w + 1], (8, 128))
            other = half_swap(spread)
            vjc_ref[(2 * vp) * VARS + w] = jnp.where(low, spread, other)
            vjc_ref[(2 * vp + 1) * VARS + w] = jnp.where(low, other, spread)
    for f2 in range(3):
        for vp in range(6):
            even = fj_ref[2 * f2 * 6 + vp]
            odd = fj_ref[(2 * f2 + 1) * 6 + vp]
            for w in range(VARS):
                fjc_ref[(f2 * 6 + vp) * VARS + w] = jnp.where(
                    lane < 64,
                    jnp.broadcast_to(even[:, w : w + 1], (8, 128)),
                    jnp.broadcast_to(odd[:, w : w + 1], (8, 128)),
                )
    stiff = stiff_ref[...]
    high = stiff.astype(BF16)
    khi_ref[...] = high
    klo_ref[...] = (stiff - high.astype(F32)).astype(BF16)


def apply_inverse(inv_ref, residual, halves):
    result = {}
    for h in range(halves):
        for v in range(VARS):
            acc = inv_ref[(v * VARS) * 2 + h] * residual[0, h]
            for w in range(1, VARS):
                acc = acc + inv_ref[(v * VARS + w) * 2 + h] * residual[w, h]
            result[v, h] = OMEGA * acc
    return result


def store_split(ref, row, column, first, second):
    both = jnp.concatenate([first, second], axis=0)
    high = both.astype(BF16)
    ref[row : row + 16, column : column + 128] = high
    ref[48 + row : 64 + row, column : column + 128] = (both - high.astype(F32)).astype(BF16)


def emit(state, halves, trace_ref, split_ref, face_ref):
    low = rows8() < 4
    for h in range(halves):
        matrix = {}
        for vp in range(6):
            matrix[vp] = pair_turn(state[2 * vp, h], state[2 * vp + 1, h], low)
        for part in range(2):
            for vq in range(3):
                store_split(split_ref, vq * 16, (2 * h + part) * 128, matrix[2 * vq][part], matrix[2 * vq + 1][part])
    width = 256 * halves
    both = jnp.dot(split_ref[:, :width], trace_ref[:width, :], preferred_element_type=F32)
    traces = both[:48] + both[48:]
    for f2 in range(3):
        face_ref[f2 * 48 : f2 * 48 + 48, :] = traces[:, f2 * 128 : f2 * 128 + 128]


def to_state(matrix, halves, low):
    state = {}
    for h in range(halves):
        for vp in range(6):
            first = matrix[vp * 8 : vp * 8 + 8, 256 * h : 256 * h + 128]
            second = matrix[vp * 8 : vp * 8 + 8, 256 * h + 128 : 256 * h + 256]
            state[2 * vp, h], state[2 * vp + 1, h] = pair_turn(first, second, low)
    return state


def residual_of(u_ref, base_ref, split_ref, own_ref, even_ref, odd_ref, start_ref, idx_ref, sign_ref,
                vjc_ref, fjc_ref, khi_ref, klo_ref, lift_ref, pool, pick0, pick1, jump_ref, halves_in, halves):
    low = rows8() < 4
    left = lanes8() < 64
    pool[0:144, :] = own_ref[...]
    pool[144:288, :] = even_ref[...]
    pool[288:432, :] = odd_ref[...]
    for face in range(6):
        target = pick1 if face % 2 else pick0
        for e in range(4):
            target[pl.ds((face // 2) * 48 + e, 12, stride=4), :] = pool[pl.ds(start_ref[face * 4 + e], 12, stride=4), :]
    for f2 in range(3):
        spread = {}
        for vp in range(6):
            at = f2 * 48 + vp * 8
            even = jnp.take_along_axis(pick0[at : at + 8, :], idx_ref[2 * f2], axis=1)
            odd = jnp.take_along_axis(pick1[at : at + 8, :], idx_ref[2 * f2 + 1], axis=1)
            jump = own_ref[at : at + 8, :] - jnp.where(left, even, odd) * sign_ref[f2]
            spread[2 * vp], spread[2 * vp + 1] = pair_turn(jump, jump, low)
        flux = []
        for vp in range(6):
            acc = fjc_ref[(f2 * 6 + vp) * VARS] * spread[0]
            for w in range(1, VARS):
                acc = acc + fjc_ref[(f2 * 6 + vp) * VARS + w] * spread[w]
            flux.append(acc)
        for vq in range(3):
            store_split(jump_ref, vq * 16, f2 * 128, flux[2 * vq], flux[2 * vq + 1])
    kin = 256 * halves_in
    kout = 256 * halves
    blended = jnp.dot(split_ref[:, :kin], khi_ref[:kin, :kout], preferred_element_type=F32)
    rest = jnp.dot(split_ref[0:48, :kin], klo_ref[:kin, :kout], preferred_element_type=F32)
    blended = to_state(blended[:48] + blended[48:] + rest, halves, low)
    lifted = jnp.dot(jump_ref[...], lift_ref[:, :kout], preferred_element_type=F32)
    lifted = to_state(lifted[:48] + lifted[48:], halves, low)
    residual = {}
    for h in range(halves):
        for v in range(VARS):
            acc = vjc_ref[v * VARS] * blended[0, h]
            for w in range(1, VARS):
                acc = acc + vjc_ref[v * VARS + w] * blended[w, h]
            residual[v, h] = base_ref[2 * v + h] - SIGMA * u_ref[2 * v + h] - acc - lifted[v, h]
    return residual


def coarse_mask():
    lane = lanes8()
    return jnp.where((((lane >> 3) & 7) < QC) & ((lane & 7) < QC), 1.0, 0.0).astype(F32)


def zero_tile():
    return jnp.zeros((8, 128), F32)


def first_body(inv_ref, rhs_ref, trace_ref, u_ref, split_ref, face_ref):
    state = apply_inverse(inv_ref, {(v, h): rhs_ref[2 * v + h] for v in range(VARS) for h in range(2)}, 2)
    for v in range(VARS):
        for h in range(2):
            u_ref[2 * v + h] = state[v, h]
    emit(state, 2, trace_ref, split_ref, face_ref)


def fine_body(inv_ref, trace_ref, u_ref, *rest):
    shared, (out_ref, split_ref, face_ref), scratch = rest[:13], rest[13:16], rest[16:]
    residual = residual_of(u_ref, *shared, *scratch, 2, 2)
    state = apply_inverse(inv_ref, residual, 2)
    for v in range(VARS):
        for h in range(2):
            state[v, h] = state[v, h] + u_ref[2 * v + h]
            out_ref[2 * v + h] = state[v, h]
    emit(state, 2, trace_ref, split_ref, face_ref)


def last_body(inv_ref, u_ref, *rest):
    shared, out_ref, scratch = rest[:13], rest[13], rest[14:]
    residual = residual_of(u_ref, *shared, *scratch, 2, 2)
    state = apply_inverse(inv_ref, residual, 2)
    for v in range(VARS):
        for h in range(2):
            out_ref[2 * v + h] = state[v, h] + u_ref[2 * v + h]


def restrict_body(inv_ref, trace_ref, u_ref, *rest):
    shared, (low_ref, out_ref, split_ref, face_ref), scratch = rest[:13], rest[13:17], rest[17:]
    residual = residual_of(u_ref, *shared, *scratch, 2, 1)
    mask = coarse_mask()
    residual = {key: tile * mask for key, tile in residual.items()}
    state = apply_inverse(inv_ref, residual, 1)
    for v in range(VARS):
        low_ref[2 * v] = residual[v, 0]
        low_ref[2 * v + 1] = zero_tile()
        out_ref[2 * v] = state[v, 0]
        out_ref[2 * v + 1] = zero_tile()
    emit(state, 1, trace_ref, split_ref, face_ref)


def coarse_body(inv_ref, trace_ref, fine_ref, u_ref, *rest):
    shared, (out_ref, split_ref, face_ref), scratch = rest[:13], rest[13:16], rest[16:]
    residual = residual_of(u_ref, *shared, *scratch, 1, 1)
    mask = coarse_mask()
    residual = {key: tile * mask for key, tile in residual.items()}
    state = apply_inverse(inv_ref, residual, 1)
    for v in range(VARS):
        state[v, 0] = state[v, 0] + u_ref[2 * v] + fine_ref[2 * v]
        state[v, 1] = fine_ref[2 * v + 1]
        out_ref[2 * v] = state[v, 0]
        out_ref[2 * v + 1] = state[v, 1]
    emit(state, 2, trace_ref, split_ref, face_ref)


STATE = VMEM((24, 8, 128), F32)
SPLIT = VMEM((96, 512), BF16)
FACES = VMEM((144, 128), F32)


def in_vmem(value):
    return pltpu.with_memory_space_constraint(value, VMEM)


def call(body, outs, args, scratch=(), smem=(), smem_outs=()):
    spec = pl.BlockSpec(memory_space=VMEM)
    scalar = pl.BlockSpec(memory_space=pltpu.SMEM)
    return pl.pallas_call(
        body,
        out_shape=list(outs),
        in_specs=[scalar if at in smem else spec for at in range(len(args))],
        out_specs=[scalar if at in smem_outs else spec for at in range(len(outs))],
        scratch_shapes=list(scratch),
        compiler_params=pltpu.CompilerParams(vmem_limit_bytes=32 * 1024 * 1024),
    )(*args)


def exchange(faces):
    count = lax.axis_size("dom")
    odd = []
    for at in range(1, count - 1, 2):
        odd += [(at, at + 1), (at + 1, at)]
    even = [(at, at ^ 1) for at in range(count)]
    from_odd = lax.ppermute(faces, "dom", odd)
    from_even = lax.ppermute(faces, "dom", even)
    return in_vmem(from_even), in_vmem(from_odd)


def local(rhs, stiffness, vol_jac, face_jac, block_inv, face_owner, face_elem, face_side, face_turn):
    me = lax.axis_index("dom").astype(jnp.int32).reshape(1)
    rhs_state = in_vmem(rhs.reshape(4, 12, 4, 128).transpose(1, 2, 0, 3).reshape(24, 8, 128))
    inverse = in_vmem(block_inv.reshape(4, 12, 12, 4, 128).transpose(1, 2, 3, 0, 4).reshape(288, 8, 128))
    vj = vol_jac.transpose(1, 0, 2).reshape(6, 8, 12)
    fj = face_jac.transpose(1, 2, 0, 3).reshape(36, 8, 12)
    trace = in_vmem(jnp.asarray(trace_matrix(), BF16))
    lift = in_vmem(jnp.asarray(lift_matrix(), BF16))

    u, split, faces = call(first_body, (STATE, SPLIT, FACES), (inverse, rhs_state, trace))
    start, idx, sign, vjc, fjc, khi, klo = call(
        prepare_body,
        (
            pltpu.SMEM((24,), jnp.int32),
            VMEM((6, 8, 128), jnp.int32),
            VMEM((3, 8, 128), F32),
            VMEM((144, 8, 128), F32),
            VMEM((216, 8, 128), F32),
            VMEM((512, 512), BF16),
            VMEM((512, 512), BF16),
        ),
        (me, face_owner, face_elem, face_side, face_turn, vj, fj, stiffness),
        smem=(0, 1, 2, 3, 4),
        smem_outs=(0,),
    )
    tables = (start, idx, sign, vjc, fjc, khi, klo, lift)
    scratch = (VMEM((432, 128), F32), FACES, FACES, VMEM((96, 384), BF16))

    def stage(body, outs, head, u, base, split, faces):
        even, odd = exchange(faces)
        args = (*head, u, base, split, faces, even, odd, *tables)
        return call(body, outs, args, scratch, smem=(len(head) + 6,))

    fine_two, split, faces = stage(fine_body, (STATE, SPLIT, FACES), (inverse, trace), u, rhs_state, split, faces)
    low_rhs, coarse, split, faces = stage(
        restrict_body, (STATE, STATE, SPLIT, FACES), (inverse, trace), fine_two, rhs_state, split, faces
    )
    u, split, faces = stage(
        coarse_body, (STATE, SPLIT, FACES), (inverse, trace, fine_two), coarse, low_rhs, split, faces
    )
    u, split, faces = stage(fine_body, (STATE, SPLIT, FACES), (inverse, trace), u, rhs_state, split, faces)
    (u,) = stage(last_body, (jax.ShapeDtypeStruct((24, 8, 128), F32),), (inverse,), u, rhs_state, split, faces)
    return u.reshape(12, 4, 4, 128).transpose(2, 0, 1, 3).reshape(4, 12, 512)


def solution(mesh):
    dom = P("dom")
    return jax.shard_map(
        local,
        mesh=mesh,
        in_specs=(dom, P(), dom, dom, dom, dom, dom, dom, dom),
        out_specs=dom,
        check_vma=False,
    )
```

```python
import jax
import jax.numpy as jnp
import numpy as np
from jax import lax
from jax.experimental import pallas as pl
from jax.experimental.pallas import tpu as pltpu
from jax.sharding import PartitionSpec as P


QF = 8
QC = 4
VARS = 12
SIGMA = 2.0
OMEGA = 0.7
F32 = jnp.float32
BF16 = jnp.bfloat16
VMEM = pltpu.VMEM


def trace_matrix():
    matrix = np.zeros((512, 384), np.float32)
    for i in range(QF):
        for j in range(QF):
            for k in range(QF):
                mode = (i * QF + j) * QF + k
                triple = (i, j, k)
                for face in range(6):
                    normal = triple[face // 2]
                    a, b = [triple[place] for place in range(3) if place != face // 2]
                    matrix[mode, face * 64 + a * 8 + b] = (-1.0) ** normal if face % 2 == 0 else 1.0
    return matrix


def low_trace_matrix():
    places = [face * 64 + a * 8 + b for face in range(6) for a in range(QC) for b in range(QC)]
    return np.pad(trace_matrix()[:, places], ((0, 0), (0, 32)))


def lift_matrix():
    degrees = np.stack(np.meshgrid(*[np.arange(QF)] * 3, indexing="ij"), -1).reshape(512, 3)
    scale = np.stack([(2.0 * degrees[:, face // 2] + 1.0) / 16.0 for face in range(6)], -1)
    return (trace_matrix().reshape(512, 6, 64) * scale[:, :, None]).reshape(512, 384).T


def rows8():
    return lax.broadcasted_iota(jnp.int32, (8, 128), 0)


def lanes8():
    return lax.broadcasted_iota(jnp.int32, (8, 128), 1)


def half_swap(tile):
    return pltpu.roll(tile, 4, axis=0)


def pair_turn(first, second, low):
    return jnp.where(low, first, half_swap(second)), jnp.where(low, half_swap(first), second)


def prepare_tables(me, owner_ref, elem_ref, side_ref, turn_ref, vj_ref, fj_ref,
                   start_ref, idx_ref, sign_ref, low_start_ref, low_idx_ref, vjc_ref, fjc_ref):
    rows = rows8()
    lane = lanes8()
    low = rows < 4
    element = rows & 3
    a = (lane >> 3) & 7
    b = lane & 7
    signs = []
    for face in range(6):
        sides = jnp.zeros((8, 128), jnp.int32)
        turns = jnp.zeros((8, 128), jnp.int32)
        present = jnp.zeros((8, 128), jnp.int32)
        for e in range(4):
            owner = owner_ref[e, face]
            side = side_ref[e, face]
            block = jnp.where(owner == me, 0, jnp.where(owner == (me ^ 1), 1, 2))
            block = jnp.where(owner < 0, 0, block)
            start_ref[face * 4 + e] = block * 144 + (side >> 1) * 48 + elem_ref[e, face]
            low_start_ref[face * 4 + e] = block * 48 + elem_ref[e, face]
            here = element == e
            turns = jnp.where(here, turn_ref[e, face], turns)
            sides = jnp.where(here, side, sides)
            present = jnp.where(here, jnp.where(owner >= 0, 1, 0), present)
        swap = (turns & 1) == 1
        idx_ref[face] = (sides & 1) * 64 + jnp.where(swap, b * 8 + a, a * 8 + b)
        low_idx_ref[face] = sides * 16 + jnp.where(swap, (b & 3) * 4 + (a & 3), (a & 3) * 4 + (b & 3))
        flips = (((turns >> 1) & a) + ((turns >> 2) & b)) & 1
        signs.append((present * (1 - 2 * flips)).astype(F32))
    for f2 in range(3):
        sign_ref[f2] = jnp.where(lane < 64, signs[2 * f2], signs[2 * f2 + 1])
    for vp in range(6):
        block = vj_ref[vp]
        for w in range(VARS):
            spread = jnp.broadcast_to(block[:, w : w + 1], (8, 128))
            other = half_swap(spread)
            vjc_ref[(2 * vp) * VARS + w] = jnp.where(low, spread, other)
            vjc_ref[(2 * vp + 1) * VARS + w] = jnp.where(low, other, spread)
    for f2 in range(3):
        for vp in range(6):
            even = fj_ref[2 * f2 * 6 + vp]
            odd = fj_ref[(2 * f2 + 1) * 6 + vp]
            for w in range(VARS):
                fjc_ref[(f2 * 6 + vp) * VARS + w] = jnp.where(
                    lane < 64,
                    jnp.broadcast_to(even[:, w : w + 1], (8, 128)),
                    jnp.broadcast_to(odd[:, w : w + 1], (8, 128)),
                )


def apply_inverse(inv_ref, residual, halves):
    result = {}
    for h in range(halves):
        for v in range(VARS):
            acc = inv_ref[(v * VARS) * 2 + h] * residual[0, h]
            for w in range(1, VARS):
                acc = acc + inv_ref[(v * VARS + w) * 2 + h] * residual[w, h]
            result[v, h] = OMEGA * acc
    return result


def store_split(ref, row, column, first, second):
    both = jnp.concatenate([first, second], axis=0)
    high = both.astype(BF16)
    ref[row : row + 16, column : column + 128] = high
    ref[48 + row : 64 + row, column : column + 128] = (both - high.astype(F32)).astype(BF16)


def emit(state, halves, trace_ref, split_ref, face_ref, low_ref=None):
    low = rows8() < 4
    for h in range(halves):
        matrix = {}
        for vp in range(6):
            matrix[vp] = pair_turn(state[2 * vp, h], state[2 * vp + 1, h], low)
        for part in range(2):
            for vq in range(3):
                store_split(split_ref, vq * 16, (2 * h + part) * 128, matrix[2 * vq][part], matrix[2 * vq + 1][part])
    width = 256 * halves
    columns = 384 if low_ref is None else 512
    both = jnp.dot(split_ref[:, :width], trace_ref[:width, :columns], preferred_element_type=F32)
    traces = both[:48] + both[48:]
    if low_ref is not None:
        low_ref[...] = traces[:, 384:]
    for f2 in range(3):
        face_ref[f2 * 48 : f2 * 48 + 48, :] = traces[:, f2 * 128 : f2 * 128 + 128]


def to_state(matrix, halves, low):
    state = {}
    for h in range(halves):
        for vp in range(6):
            first = matrix[vp * 8 : vp * 8 + 8, 256 * h : 256 * h + 128]
            second = matrix[vp * 8 : vp * 8 + 8, 256 * h + 128 : 256 * h + 256]
            state[2 * vp, h], state[2 * vp + 1, h] = pair_turn(first, second, low)
    return state


def residual_of(u_ref, base_ref, split_ref, own_ref, mine_ref, even_ref, odd_ref, start_ref, idx_ref, sign_ref,
                vjc_ref, fjc_ref, khi_ref, klo_ref, lift_ref, pool, pick0, pick1, jump_ref, halves_in, halves):
    low = rows8() < 4
    left = lanes8() < 64
    size = mine_ref.shape[0]
    pool[0:size, :] = mine_ref[...]
    pool[size : 2 * size, :] = even_ref[...]
    pool[2 * size : 3 * size, :] = odd_ref[...]
    for face in range(6):
        target = pick1 if face % 2 else pick0
        for e in range(4):
            target[pl.ds((face // 2) * 48 + e, 12, stride=4), :] = pool[pl.ds(start_ref[face * 4 + e], 12, stride=4), :]
    for f2 in range(3):
        spread = {}
        for vp in range(6):
            at = f2 * 48 + vp * 8
            even = jnp.take_along_axis(pick0[at : at + 8, :], idx_ref[2 * f2], axis=1)
            odd = jnp.take_along_axis(pick1[at : at + 8, :], idx_ref[2 * f2 + 1], axis=1)
            jump = own_ref[at : at + 8, :] - jnp.where(left, even, odd) * sign_ref[f2]
            spread[2 * vp], spread[2 * vp + 1] = pair_turn(jump, jump, low)
        flux = []
        for vp in range(6):
            acc = fjc_ref[(f2 * 6 + vp) * VARS] * spread[0]
            for w in range(1, VARS):
                acc = acc + fjc_ref[(f2 * 6 + vp) * VARS + w] * spread[w]
            flux.append(acc)
        for vq in range(3):
            store_split(jump_ref, vq * 16, f2 * 128, flux[2 * vq], flux[2 * vq + 1])
    kin = 256 * halves_in
    kout = 256 * halves
    blended = jnp.dot(split_ref[:, :kin], khi_ref[:kin, :kout], preferred_element_type=F32)
    rest = jnp.dot(split_ref[0:48, :kin], klo_ref[:kin, :kout], preferred_element_type=F32)
    blended = to_state(blended[:48] + blended[48:] + rest, halves, low)
    lifted = jnp.dot(jump_ref[...], lift_ref[:, :kout], preferred_element_type=F32)
    lifted = to_state(lifted[:48] + lifted[48:], halves, low)
    residual = {}
    for h in range(halves):
        for v in range(VARS):
            acc = vjc_ref[v * VARS] * blended[0, h]
            for w in range(1, VARS):
                acc = acc + vjc_ref[v * VARS + w] * blended[w, h]
            residual[v, h] = base_ref[2 * v + h] - SIGMA * u_ref[2 * v + h] - acc - lifted[v, h]
    return residual


def coarse_mask():
    lane = lanes8()
    return jnp.where((((lane >> 3) & 7) < QC) & ((lane & 7) < QC), 1.0, 0.0).astype(F32)


def zero_tile():
    return jnp.zeros((8, 128), F32)


def first_body(me_ref, *refs):
    sources, outs, targets, sems = refs[:11], refs[11:23], refs[23:34], refs[34]
    owner_ref, elem_ref, side_ref, turn_ref, vj_ref, fj_ref, inv_ref, rhs_ref, trace_ref, stiff_ref, lift_ref = targets
    u_ref, split_ref, face_ref, khi_ref, klo_ref = *outs[:3], *outs[10:]
    copies = [pltpu.make_async_copy(sources[at], targets[at], sems.at[at]) for at in range(11)]
    for copy in copies:
        copy.start()
    for copy in copies[:6]:
        copy.wait()
    prepare_tables(me_ref[0], owner_ref, elem_ref, side_ref, turn_ref, vj_ref, fj_ref, *outs[3:10])
    for copy in copies[6:8]:
        copy.wait()
    state = apply_inverse(inv_ref, {(v, h): rhs_ref[2 * v + h] for v in range(VARS) for h in range(2)}, 2)
    for v in range(VARS):
        for h in range(2):
            u_ref[2 * v + h] = state[v, h]
    copies[8].wait()
    emit(state, 2, trace_ref, split_ref, face_ref)
    copies[9].wait()
    stiff = stiff_ref[...]
    high = stiff.astype(BF16)
    khi_ref[...] = high
    klo_ref[...] = (stiff - high.astype(F32)).astype(BF16)
    copies[10].wait()


def fine_body(inv_ref, trace_ref, u_ref, *rest):
    fine_step(inv_ref, trace_ref, u_ref, rest[:14], *rest[14:17], None, rest[17:])


def fine_low_body(inv_ref, trace_ref, u_ref, *rest):
    fine_step(inv_ref, trace_ref, u_ref, rest[:14], *rest[14:18], rest[18:])


def fine_step(inv_ref, trace_ref, u_ref, shared, out_ref, split_ref, face_ref, low_ref, scratch):
    residual = residual_of(u_ref, *shared, *scratch, 2, 2)
    state = apply_inverse(inv_ref, residual, 2)
    for v in range(VARS):
        for h in range(2):
            state[v, h] = state[v, h] + u_ref[2 * v + h]
            out_ref[2 * v + h] = state[v, h]
    emit(state, 2, trace_ref, split_ref, face_ref, low_ref)


def last_body(inv_ref, u_ref, *rest):
    shared, out_ref, scratch = rest[:14], rest[14], rest[15:]
    residual = residual_of(u_ref, *shared, *scratch, 2, 2)
    state = apply_inverse(inv_ref, residual, 2)
    for v in range(VARS):
        for h in range(2):
            out_ref[2 * v + h] = state[v, h] + u_ref[2 * v + h]


def restrict_body(inv_ref, trace_ref, u_ref, *rest):
    shared, (low_ref, out_ref, split_ref, face_ref, mine_ref), scratch = rest[:14], rest[14:19], rest[19:]
    residual = residual_of(u_ref, *shared, *scratch, 2, 1)
    mask = coarse_mask()
    residual = {key: tile * mask for key, tile in residual.items()}
    state = apply_inverse(inv_ref, residual, 1)
    for v in range(VARS):
        low_ref[2 * v] = residual[v, 0]
        low_ref[2 * v + 1] = zero_tile()
        out_ref[2 * v] = state[v, 0]
        out_ref[2 * v + 1] = zero_tile()
    emit(state, 1, trace_ref, split_ref, face_ref, mine_ref)


def coarse_body(inv_ref, trace_ref, fine_ref, u_ref, *rest):
    shared, (out_ref, split_ref, face_ref), scratch = rest[:14], rest[14:17], rest[17:]
    residual = residual_of(u_ref, *shared, *scratch, 1, 1)
    mask = coarse_mask()
    residual = {key: tile * mask for key, tile in residual.items()}
    state = apply_inverse(inv_ref, residual, 1)
    for v in range(VARS):
        state[v, 0] = state[v, 0] + u_ref[2 * v] + fine_ref[2 * v]
        state[v, 1] = fine_ref[2 * v + 1]
        out_ref[2 * v] = state[v, 0]
        out_ref[2 * v + 1] = state[v, 1]
    emit(state, 2, trace_ref, split_ref, face_ref)


STATE = VMEM((24, 8, 128), F32)
SPLIT = VMEM((96, 512), BF16)
FACES = VMEM((144, 128), F32)
LOW_FACES = VMEM((48, 128), F32)


def in_vmem(value):
    return pltpu.with_memory_space_constraint(value, VMEM)


def call(body, outs, args, scratch=(), smem=(), smem_outs=(), far=False):
    spec = pl.BlockSpec(memory_space=VMEM)
    source = pl.BlockSpec(memory_space=pl.ANY) if far else spec
    scalar = pl.BlockSpec(memory_space=pltpu.SMEM)
    return pl.pallas_call(
        body,
        out_shape=list(outs),
        in_specs=[scalar if at in smem else source for at in range(len(args))],
        out_specs=[scalar if at in smem_outs else spec for at in range(len(outs))],
        scratch_shapes=list(scratch),
        compiler_params=pltpu.CompilerParams(vmem_limit_bytes=6 * 1024 * 1024),
    )(*args)


def exchange(faces):
    count = lax.axis_size("dom")
    odd = []
    for at in range(1, count - 1, 2):
        odd += [(at, at + 1), (at + 1, at)]
    even = [(at, at ^ 1) for at in range(count)]
    from_odd = lax.ppermute(faces, "dom", odd)
    from_even = lax.ppermute(faces, "dom", even)
    return in_vmem(from_even), in_vmem(from_odd)


def local(rhs, stiffness, vol_jac, face_jac, block_inv, face_owner, face_elem, face_side, face_turn):
    me = lax.axis_index("dom").astype(jnp.int32).reshape(1)
    rhs_state = rhs.reshape(4, 12, 4, 128).transpose(1, 2, 0, 3).reshape(24, 8, 128)
    inverse = block_inv.reshape(4, 12, 12, 4, 128).transpose(1, 2, 3, 0, 4).reshape(288, 8, 128)
    vj = vol_jac.transpose(1, 0, 2).reshape(6, 8, 12)
    fj = face_jac.transpose(1, 2, 0, 3).reshape(36, 8, 12)
    trace = jnp.asarray(np.concatenate([trace_matrix(), low_trace_matrix()], 1), BF16)
    lift = jnp.asarray(lift_matrix(), BF16)
    loads = (face_owner, face_elem, face_side, face_turn, vj, fj, inverse, rhs_state, trace, stiffness, lift)
    u, split, faces, start, idx, sign, low_start, low_idx, vjc, fjc, khi, klo, *loads = call(
        first_body,
        (
            STATE,
            SPLIT,
            FACES,
            pltpu.SMEM((24,), jnp.int32),
            VMEM((6, 8, 128), jnp.int32),
            VMEM((3, 8, 128), F32),
            pltpu.SMEM((24,), jnp.int32),
            VMEM((6, 8, 128), jnp.int32),
            VMEM((144, 8, 128), F32),
            VMEM((216, 8, 128), F32),
            VMEM((512, 512), BF16),
            VMEM((512, 512), BF16),
            *((pltpu.SMEM if at < 4 else VMEM)(load.shape, load.dtype) for at, load in enumerate(loads)),
        ),
        (me, *(pltpu.with_memory_space_constraint(load, pltpu.HBM) for load in loads)),
        (pltpu.SemaphoreType.DMA((len(loads),)),),
        smem=(0,),
        smem_outs=(3, 6, 12, 13, 14, 15),
        far=True,
    )
    inverse, rhs_state, trace, stiffness, lift = loads[6:]
    tables = (sign, vjc, fjc, khi, klo, lift)
    scratch = (VMEM((432, 128), F32), FACES, FACES, VMEM((96, 384), BF16))

    def stage(body, outs, head, u, base, split, faces, sent=None):
        low = sent is not None
        sent = sent if low else faces
        even, odd = exchange(sent)
        places = (low_start, low_idx) if low else (start, idx)
        args = (*head, u, base, split, faces, sent, even, odd, *places, *tables)
        return call(body, outs, args, scratch, smem=(len(head) + 7,))

    fine_two, split, faces, sent = stage(
        fine_low_body, (STATE, SPLIT, FACES, LOW_FACES), (inverse, trace), u, rhs_state, split, faces
    )
    low_rhs, coarse, split, faces, sent = stage(
        restrict_body,
        (STATE, STATE, SPLIT, FACES, LOW_FACES),
        (inverse, trace),
        fine_two,
        rhs_state,
        split,
        faces,
        sent,
    )
    u, split, faces = stage(
        coarse_body, (STATE, SPLIT, FACES), (inverse, trace, fine_two), coarse, low_rhs, split, faces, sent
    )
    u, split, faces = stage(fine_body, (STATE, SPLIT, FACES), (inverse, trace), u, rhs_state, split, faces)
    (u,) = stage(last_body, (jax.ShapeDtypeStruct((24, 8, 128), F32),), (inverse,), u, rhs_state, split, faces)
    return u.reshape(12, 4, 4, 128).transpose(2, 0, 1, 3).reshape(4, 12, 512)


def solution(mesh):
    dom = P("dom")
    return jax.shard_map(
        local,
        mesh=mesh,
        in_specs=(dom, P(), dom, dom, dom, dom, dom, dom, dom),
        out_specs=dom,
        check_vma=False,
    )
```

```python
import jax
import jax.numpy as jnp
import numpy as np
from jax import lax
from jax.experimental import pallas as pl
from jax.experimental.pallas import tpu as pltpu
from jax.sharding import PartitionSpec as P


QF = 8
QC = 4
VARS = 12
SIGMA = 2.0
OMEGA = 0.7
F32 = jnp.float32
BF16 = jnp.bfloat16
VMEM = pltpu.VMEM


def trace_matrix():
    matrix = np.zeros((512, 384), np.float32)
    for i in range(QF):
        for j in range(QF):
            for k in range(QF):
                mode = (i * QF + j) * QF + k
                triple = (i, j, k)
                for face in range(6):
                    normal = triple[face // 2]
                    a, b = [triple[place] for place in range(3) if place != face // 2]
                    matrix[mode, face * 64 + a * 8 + b] = (-1.0) ** normal if face % 2 == 0 else 1.0
    return matrix


def low_trace_matrix():
    places = [face * 64 + a * 8 + b for face in range(6) for a in range(QC) for b in range(QC)]
    return np.pad(trace_matrix()[:, places], ((0, 0), (0, 32)))


def lift_matrix():
    degrees = np.stack(np.meshgrid(*[np.arange(QF)] * 3, indexing="ij"), -1).reshape(512, 3)
    scale = np.stack([(2.0 * degrees[:, face // 2] + 1.0) / 16.0 for face in range(6)], -1)
    return (trace_matrix().reshape(512, 6, 64) * scale[:, :, None]).reshape(512, 384).T


def rows8():
    return lax.broadcasted_iota(jnp.int32, (8, 128), 0)


def lanes8():
    return lax.broadcasted_iota(jnp.int32, (8, 128), 1)


def half_swap(tile):
    return pltpu.roll(tile, 4, axis=0)


def pair_turn(first, second, low):
    return jnp.where(low, first, half_swap(second)), jnp.where(low, half_swap(first), second)


def prepare_tables(me, owner_ref, elem_ref, side_ref, turn_ref, vj_ref, fj_ref,
                   start_ref, idx_ref, sign_ref, low_start_ref, low_idx_ref, vjc_ref, fjc_ref):
    rows = rows8()
    lane = lanes8()
    low = rows < 4
    element = rows & 3
    a = (lane >> 3) & 7
    b = lane & 7
    signs = []
    for face in range(6):
        sides = jnp.zeros((8, 128), jnp.int32)
        turns = jnp.zeros((8, 128), jnp.int32)
        present = jnp.zeros((8, 128), jnp.int32)
        for e in range(4):
            owner = owner_ref[e, face]
            side = side_ref[e, face]
            block = jnp.where(owner == me, 0, jnp.where(owner == (me ^ 1), 1, 2))
            block = jnp.where(owner < 0, 0, block)
            start_ref[face * 4 + e] = block * 144 + (side >> 1) * 48 + elem_ref[e, face]
            low_start_ref[face * 4 + e] = block * 48 + elem_ref[e, face]
            here = element == e
            turns = jnp.where(here, turn_ref[e, face], turns)
            sides = jnp.where(here, side, sides)
            present = jnp.where(here, jnp.where(owner >= 0, 1, 0), present)
        swap = (turns & 1) == 1
        idx_ref[face] = (sides & 1) * 64 + jnp.where(swap, b * 8 + a, a * 8 + b)
        low_idx_ref[face] = sides * 16 + jnp.where(swap, (b & 3) * 4 + (a & 3), (a & 3) * 4 + (b & 3))
        flips = (((turns >> 1) & a) + ((turns >> 2) & b)) & 1
        signs.append((present * (1 - 2 * flips)).astype(F32))
    for f2 in range(3):
        sign_ref[f2] = jnp.where(lane < 64, signs[2 * f2], signs[2 * f2 + 1])
    for vp in range(6):
        block = vj_ref[vp]
        for w in range(VARS):
            spread = jnp.broadcast_to(block[:, w : w + 1], (8, 128))
            other = half_swap(spread)
            vjc_ref[(2 * vp) * VARS + w] = jnp.where(low, spread, other)
            vjc_ref[(2 * vp + 1) * VARS + w] = jnp.where(low, other, spread)
    for f2 in range(3):
        for vp in range(6):
            even = fj_ref[2 * f2 * 6 + vp]
            odd = fj_ref[(2 * f2 + 1) * 6 + vp]
            for w in range(VARS):
                fjc_ref[(f2 * 6 + vp) * VARS + w] = jnp.where(
                    lane < 64,
                    jnp.broadcast_to(even[:, w : w + 1], (8, 128)),
                    jnp.broadcast_to(odd[:, w : w + 1], (8, 128)),
                )


def apply_inverse(inv_ref, residual, halves):
    result = {}
    for h in range(halves):
        for v in range(VARS):
            acc = inv_ref[(v * VARS) * 2 + h] * residual[0, h]
            for w in range(1, VARS):
                acc = acc + inv_ref[(v * VARS + w) * 2 + h] * residual[w, h]
            result[v, h] = OMEGA * acc
    return result


def store_split(ref, row, column, first, second):
    both = jnp.concatenate([first, second], axis=0)
    high = both.astype(BF16)
    ref[row : row + 16, column : column + 128] = high
    ref[48 + row : 64 + row, column : column + 128] = (both - high.astype(F32)).astype(BF16)


def emit(state, halves, trace_ref, split_ref, face_ref, low_ref=None):
    low = rows8() < 4
    for h in range(halves):
        matrix = {}
        for vp in range(6):
            matrix[vp] = pair_turn(state[2 * vp, h], state[2 * vp + 1, h], low)
        for part in range(2):
            for vq in range(3):
                store_split(split_ref, vq * 16, (2 * h + part) * 128, matrix[2 * vq][part], matrix[2 * vq + 1][part])
    width = 256 * halves
    columns = 384 if low_ref is None else 512
    both = jnp.dot(split_ref[:, :width], trace_ref[:width, :columns], preferred_element_type=F32)
    traces = both[:48] + both[48:]
    if low_ref is not None:
        low_ref[...] = traces[:, 384:]
    for f2 in range(3):
        face_ref[f2 * 48 : f2 * 48 + 48, :] = traces[:, f2 * 128 : f2 * 128 + 128]


def to_state(matrix, halves, low):
    state = {}
    for h in range(halves):
        for vp in range(6):
            first = matrix[vp * 8 : vp * 8 + 8, 256 * h : 256 * h + 128]
            second = matrix[vp * 8 : vp * 8 + 8, 256 * h + 128 : 256 * h + 256]
            state[2 * vp, h], state[2 * vp + 1, h] = pair_turn(first, second, low)
    return state


def residual_of(u_ref, base_ref, split_ref, own_ref, mine_ref, even_ref, odd_ref, start_ref, idx_ref, sign_ref,
                vjc_ref, fjc_ref, khi_ref, klo_ref, lift_ref, pool, pick0, pick1, jump_ref, halves_in, halves):
    low = rows8() < 4
    left = lanes8() < 64
    size = mine_ref.shape[0]
    pool[0:size, :] = mine_ref[...]
    pool[size : 2 * size, :] = even_ref[...]
    pool[2 * size : 3 * size, :] = odd_ref[...]
    for face in range(6):
        target = pick1 if face % 2 else pick0
        for e in range(4):
            target[pl.ds((face // 2) * 48 + e, 12, stride=4), :] = pool[pl.ds(start_ref[face * 4 + e], 12, stride=4), :]
    for f2 in range(3):
        spread = {}
        for vp in range(6):
            at = f2 * 48 + vp * 8
            even = jnp.take_along_axis(pick0[at : at + 8, :], idx_ref[2 * f2], axis=1)
            odd = jnp.take_along_axis(pick1[at : at + 8, :], idx_ref[2 * f2 + 1], axis=1)
            jump = own_ref[at : at + 8, :] - jnp.where(left, even, odd) * sign_ref[f2]
            spread[2 * vp], spread[2 * vp + 1] = pair_turn(jump, jump, low)
        flux = []
        for vp in range(6):
            acc = fjc_ref[(f2 * 6 + vp) * VARS] * spread[0]
            for w in range(1, VARS):
                acc = acc + fjc_ref[(f2 * 6 + vp) * VARS + w] * spread[w]
            flux.append(acc)
        for vq in range(3):
            store_split(jump_ref, vq * 16, f2 * 128, flux[2 * vq], flux[2 * vq + 1])
    kin = 256 * halves_in
    kout = 256 * halves
    blended = jnp.dot(split_ref[:, :kin], khi_ref[:kin, :kout], preferred_element_type=F32)
    rest = jnp.dot(split_ref[0:48, :kin], klo_ref[:kin, :kout], preferred_element_type=F32)
    blended = to_state(blended[:48] + blended[48:] + rest, halves, low)
    lifted = jnp.dot(jump_ref[...], lift_ref[:, :kout], preferred_element_type=F32)
    lifted = to_state(lifted[:48] + lifted[48:], halves, low)
    residual = {}
    for h in range(halves):
        for v in range(VARS):
            acc = vjc_ref[v * VARS] * blended[0, h]
            for w in range(1, VARS):
                acc = acc + vjc_ref[v * VARS + w] * blended[w, h]
            residual[v, h] = base_ref[2 * v + h] - SIGMA * u_ref[2 * v + h] - acc - lifted[v, h]
    return residual


def coarse_mask():
    lane = lanes8()
    return jnp.where((((lane >> 3) & 7) < QC) & ((lane & 7) < QC), 1.0, 0.0).astype(F32)


def zero_tile():
    return jnp.zeros((8, 128), F32)


def start_all(sources, targets, sems):
    copies = [pltpu.make_async_copy(source, target, sems.at[at]) for at, (source, target) in enumerate(zip(sources, targets))]
    for copy in copies:
        copy.start()
    return copies


def first_body(*refs):
    sources, (u_ref, split_ref, face_ref), targets, sems = refs[:3], refs[3:6], refs[6:9], refs[9]
    inv_ref, rhs_ref, trace_ref = targets
    copies = start_all(sources, targets, sems)
    copies[0].wait()
    copies[1].wait()
    state = apply_inverse(inv_ref, {(v, h): rhs_ref[2 * v + h] for v in range(VARS) for h in range(2)}, 2)
    for v in range(VARS):
        for h in range(2):
            u_ref[2 * v + h] = state[v, h]
    copies[2].wait()
    emit(state, 2, trace_ref, split_ref, face_ref)


def prepare_body(me_ref, *refs):
    sources, tables, (khi_ref, klo_ref, lift_ref) = refs[:8], refs[8:15], refs[15:18]
    owner_ref, elem_ref, side_ref, turn_ref, vj_ref, fj_ref, stiff_ref, sems = refs[18:]
    copies = start_all(sources, (owner_ref, elem_ref, side_ref, turn_ref, vj_ref, fj_ref, stiff_ref, lift_ref), sems)
    for copy in copies[:6]:
        copy.wait()
    prepare_tables(me_ref[0], owner_ref, elem_ref, side_ref, turn_ref, vj_ref, fj_ref, *tables)
    copies[6].wait()
    stiff = stiff_ref[...]
    high = stiff.astype(BF16)
    khi_ref[...] = high
    klo_ref[...] = (stiff - high.astype(F32)).astype(BF16)
    copies[7].wait()


def fine_body(inv_ref, trace_ref, u_ref, *rest):
    fine_step(inv_ref, trace_ref, u_ref, rest[:14], *rest[14:17], None, rest[17:])


def fine_low_body(inv_ref, trace_ref, u_ref, *rest):
    fine_step(inv_ref, trace_ref, u_ref, rest[:14], *rest[14:18], rest[18:])


def fine_step(inv_ref, trace_ref, u_ref, shared, out_ref, split_ref, face_ref, low_ref, scratch):
    residual = residual_of(u_ref, *shared, *scratch, 2, 2)
    state = apply_inverse(inv_ref, residual, 2)
    for v in range(VARS):
        for h in range(2):
            state[v, h] = state[v, h] + u_ref[2 * v + h]
            out_ref[2 * v + h] = state[v, h]
    emit(state, 2, trace_ref, split_ref, face_ref, low_ref)


def last_body(inv_ref, u_ref, *rest):
    shared, out_hbm, scratch, out_ref, sems = rest[:14], rest[14], rest[15:19], rest[19], rest[20]
    residual = residual_of(u_ref, *shared, *scratch, 2, 2)
    copies = []
    for part in range(3):
        for v in range(4 * part, 4 * part + 4):
            for h in range(2):
                acc = inv_ref[(v * VARS) * 2 + h] * residual[0, h]
                for w in range(1, VARS):
                    acc = acc + inv_ref[(v * VARS + w) * 2 + h] * residual[w, h]
                out_ref[2 * v + h] = OMEGA * acc + u_ref[2 * v + h]
        piece = pl.ds(8 * part, 8)
        copies.append(pltpu.make_async_copy(out_ref.at[piece], out_hbm.at[piece], sems.at[part]))
        copies[-1].start()
    for copy in copies:
        copy.wait()


def restrict_body(inv_ref, trace_ref, u_ref, *rest):
    shared, (low_ref, out_ref, split_ref, face_ref, mine_ref), scratch = rest[:14], rest[14:19], rest[19:]
    residual = residual_of(u_ref, *shared, *scratch, 2, 1)
    mask = coarse_mask()
    residual = {key: tile * mask for key, tile in residual.items()}
    state = apply_inverse(inv_ref, residual, 1)
    for v in range(VARS):
        low_ref[2 * v] = residual[v, 0]
        low_ref[2 * v + 1] = zero_tile()
        out_ref[2 * v] = state[v, 0]
        out_ref[2 * v + 1] = zero_tile()
    emit(state, 1, trace_ref, split_ref, face_ref, mine_ref)


def coarse_body(inv_ref, trace_ref, fine_ref, u_ref, *rest):
    shared, (out_ref, split_ref, face_ref), scratch = rest[:14], rest[14:17], rest[17:]
    residual = residual_of(u_ref, *shared, *scratch, 1, 1)
    mask = coarse_mask()
    residual = {key: tile * mask for key, tile in residual.items()}
    state = apply_inverse(inv_ref, residual, 1)
    for v in range(VARS):
        state[v, 0] = state[v, 0] + u_ref[2 * v] + fine_ref[2 * v]
        state[v, 1] = fine_ref[2 * v + 1]
        out_ref[2 * v] = state[v, 0]
        out_ref[2 * v + 1] = state[v, 1]
    emit(state, 2, trace_ref, split_ref, face_ref)


STATE = VMEM((24, 8, 128), F32)
SPLIT = VMEM((96, 512), BF16)
FACES = VMEM((144, 128), F32)
LOW_FACES = VMEM((48, 128), F32)


def in_vmem(value):
    return pltpu.with_memory_space_constraint(value, VMEM)


def in_hbm(value):
    return pltpu.with_memory_space_constraint(value, pltpu.HBM)


def call(body, outs, args, scratch=(), smem=(), smem_outs=(), far=False, far_out=False):
    spec = pl.BlockSpec(memory_space=VMEM)
    source = pl.BlockSpec(memory_space=pl.ANY) if far else spec
    target = pl.BlockSpec(memory_space=pl.ANY) if far_out else spec
    scalar = pl.BlockSpec(memory_space=pltpu.SMEM)
    return pl.pallas_call(
        body,
        out_shape=list(outs),
        in_specs=[scalar if at in smem else source for at in range(len(args))],
        out_specs=[scalar if at in smem_outs else target for at in range(len(outs))],
        scratch_shapes=list(scratch),
        compiler_params=pltpu.CompilerParams(vmem_limit_bytes=6 * 1024 * 1024),
    )(*args)


def exchange(faces):
    count = lax.axis_size("dom")
    odd = []
    for at in range(1, count - 1, 2):
        odd += [(at, at + 1), (at + 1, at)]
    even = [(at, at ^ 1) for at in range(count)]
    from_odd = lax.ppermute(faces, "dom", odd)
    from_even = lax.ppermute(faces, "dom", even)
    return in_vmem(from_even), in_vmem(from_odd)


def local(rhs, stiffness, vol_jac, face_jac, block_inv, face_owner, face_elem, face_side, face_turn):
    me = lax.axis_index("dom").astype(jnp.int32).reshape(1)
    rhs_state = rhs.reshape(4, 12, 4, 128).transpose(1, 2, 0, 3).reshape(24, 8, 128)
    inverse = block_inv.reshape(4, 12, 12, 4, 128).transpose(1, 2, 3, 0, 4).reshape(288, 8, 128)
    vj = vol_jac.transpose(1, 0, 2).reshape(6, 8, 12)
    fj = face_jac.transpose(1, 2, 0, 3).reshape(36, 8, 12)
    trace = jnp.asarray(np.concatenate([trace_matrix(), low_trace_matrix()], 1), BF16)
    lift = jnp.asarray(lift_matrix(), BF16)
    loads = (inverse, rhs_state, trace)
    u, split, faces, inverse, rhs_state, trace = call(
        first_body,
        (STATE, SPLIT, FACES, *(VMEM(load.shape, load.dtype) for load in loads)),
        tuple(in_hbm(load) for load in loads),
        (pltpu.SemaphoreType.DMA((3,)),),
        far=True,
    )
    loads = (face_owner, face_elem, face_side, face_turn, vj, fj, stiffness, lift)
    start, idx, sign, low_start, low_idx, vjc, fjc, khi, klo, lift = call(
        prepare_body,
        (
            pltpu.SMEM((24,), jnp.int32),
            VMEM((6, 8, 128), jnp.int32),
            VMEM((3, 8, 128), F32),
            pltpu.SMEM((24,), jnp.int32),
            VMEM((6, 8, 128), jnp.int32),
            VMEM((144, 8, 128), F32),
            VMEM((216, 8, 128), F32),
            VMEM((512, 512), BF16),
            VMEM((512, 512), BF16),
            VMEM((384, 512), BF16),
        ),
        (me, *(in_hbm(load) for load in loads)),
        (
            *(pltpu.SMEM((4, 6), jnp.int32) for _ in range(4)),
            VMEM((6, 8, 12), F32),
            VMEM((36, 8, 12), F32),
            VMEM((512, 512), F32),
            pltpu.SemaphoreType.DMA((8,)),
        ),
        smem=(0,),
        smem_outs=(0, 3),
        far=True,
    )
    tables = (sign, vjc, fjc, khi, klo, lift)
    scratch = (VMEM((432, 128), F32), FACES, FACES, VMEM((96, 384), BF16))

    def stage(body, outs, head, u, base, split, faces, sent=None, more=(), far_out=False):
        low = sent is not None
        sent = sent if low else faces
        even, odd = exchange(sent)
        places = (low_start, low_idx) if low else (start, idx)
        args = (*head, u, base, split, faces, sent, even, odd, *places, *tables)
        return call(body, outs, args, (*scratch, *more), smem=(len(head) + 7,), far_out=far_out)

    fine_two, split, faces, sent = stage(
        fine_low_body, (STATE, SPLIT, FACES, LOW_FACES), (inverse, trace), u, rhs_state, split, faces
    )
    low_rhs, coarse, split, faces, sent = stage(
        restrict_body,
        (STATE, STATE, SPLIT, FACES, LOW_FACES),
        (inverse, trace),
        fine_two,
        rhs_state,
        split,
        faces,
        sent,
    )
    u, split, faces = stage(
        coarse_body, (STATE, SPLIT, FACES), (inverse, trace, fine_two), coarse, low_rhs, split, faces, sent
    )
    u, split, faces = stage(fine_body, (STATE, SPLIT, FACES), (inverse, trace), u, rhs_state, split, faces)
    (u,) = stage(
        last_body,
        (jax.ShapeDtypeStruct((24, 8, 128), F32),),
        (inverse,),
        u,
        rhs_state,
        split,
        faces,
        more=(STATE, pltpu.SemaphoreType.DMA((3,))),
        far_out=True,
    )
    return u.reshape(12, 4, 4, 128).transpose(2, 0, 1, 3).reshape(4, 12, 512)


def solution(mesh):
    dom = P("dom")
    return jax.shard_map(
        local,
        mesh=mesh,
        in_specs=(dom, P(), dom, dom, dom, dom, dom, dom, dom),
        out_specs=dom,
        check_vma=False,
    )
```

```python
import jax
import jax.numpy as jnp
import numpy as np
from jax import lax
from jax.experimental import pallas as pl
from jax.experimental.pallas import tpu as pltpu
from jax.sharding import PartitionSpec as P


QF = 8
QC = 4
VARS = 12
FLUX_ROW = 144 + 288
NUMBER_ROW = FLUX_ROW + 40
MESSAGE_ROWS = NUMBER_ROW + 16
SIGMA = 2.0
OMEGA = 0.7
F32 = jnp.float32
BF16 = jnp.bfloat16
VMEM = pltpu.VMEM


def trace_matrix():
    matrix = np.zeros((512, 384), np.float32)
    for i in range(QF):
        for j in range(QF):
            for k in range(QF):
                mode = (i * QF + j) * QF + k
                triple = (i, j, k)
                for face in range(6):
                    normal = triple[face // 2]
                    a, b = [triple[place] for place in range(3) if place != face // 2]
                    matrix[mode, face * 64 + a * 8 + b] = (-1.0) ** normal if face % 2 == 0 else 1.0
    return matrix


def low_trace_matrix():
    places = [face * 64 + a * 8 + b for face in range(6) for a in range(QC) for b in range(QC)]
    return np.pad(trace_matrix()[:, places], ((0, 0), (0, 32)))


def lift_matrix():
    degrees = np.stack(np.meshgrid(*[np.arange(QF)] * 3, indexing="ij"), -1).reshape(512, 3)
    scale = np.stack([(2.0 * degrees[:, face // 2] + 1.0) / 16.0 for face in range(6)], -1)
    return (trace_matrix().reshape(512, 6, 64) * scale[:, :, None]).reshape(512, 384).T


def rows8():
    return lax.broadcasted_iota(jnp.int32, (8, 128), 0)


def lanes8():
    return lax.broadcasted_iota(jnp.int32, (8, 128), 1)


def half_swap(tile):
    return pltpu.roll(tile, 4, axis=0)


def pair_turn(first, second, low):
    return jnp.where(low, first, half_swap(second)), jnp.where(low, half_swap(first), second)


def face_tables(other, number, start_ref, low_start_ref, idx_ref, low_idx_ref, block_of, masks):
    owner_of, elem_of, side_of, turn_of = number
    rows = rows8()
    lane = lanes8()
    element = rows & 3
    a = (lane >> 3) & 7
    b = lane & 7
    signs = []
    for face in range(6):
        sides = jnp.zeros((8, 128), jnp.int32)
        turns = jnp.zeros((8, 128), jnp.int32)
        here_far = jnp.zeros((8, 128), jnp.int32)
        here_near = jnp.zeros((8, 128), jnp.int32)
        for e in range(4):
            owner = owner_of(e, face)
            side = side_of(e, face)
            elem = elem_of(e, face)
            block = block_of(owner)
            start_ref[face * 4 + e] = block * 144 + (side >> 1) * 48 + elem
            low_start_ref[face * 4 + e] = block * 48 + elem
            masks(face * 4 + e, (side >> 1) * 48 + elem, elem)
            here = element == e
            turns = jnp.where(here, turn_of(e, face), turns)
            sides = jnp.where(here, side, sides)
            far = jnp.where((owner >= 0) & (owner == other), 1, 0)
            here_far = jnp.where(here, far, here_far)
            here_near = jnp.where(here, jnp.where(owner >= 0, 1, 0) - far, here_near)
        swap = (turns & 1) == 1
        idx_ref[face] = (sides & 1) * 64 + jnp.where(swap, b * 8 + a, a * 8 + b)
        low_idx_ref[face] = sides * 16 + jnp.where(swap, (b & 3) * 4 + (a & 3), (a & 3) * 4 + (b & 3))
        flips = 1 - 2 * ((((turns >> 1) & a) + ((turns >> 2) & b)) & 1)
        signs.append(((here_near * flips).astype(F32), (here_far * flips).astype(F32)))
    return signs


def flux_table(block_of, fjc_ref):
    left = lanes8() < 64
    for f2 in range(3):
        for vp in range(6):
            even = block_of(2 * f2 * 6 + vp)
            odd = block_of((2 * f2 + 1) * 6 + vp)
            for w in range(VARS):
                fjc_ref[(f2 * 6 + vp) * VARS + w] = jnp.where(
                    left,
                    jnp.broadcast_to(even[:, w : w + 1], (8, 128)),
                    jnp.broadcast_to(odd[:, w : w + 1], (8, 128)),
                )


def odd_partner(me):
    return me - 1 + 2 * (me & 1)


def prepare_tables(me, owner_ref, elem_ref, side_ref, turn_ref, vj_ref, fj_ref, start_ref, idx_ref, sign_ref,
                   low_start_ref, low_idx_ref, near_ref, far_ref, plain_ref, low_plain_ref, vjc_ref, fjc_ref):
    left = lanes8() < 64
    low = rows8() < 4

    def block_of(owner):
        block = jnp.where(owner == me, 0, jnp.where(owner == (me ^ 1), 1, 2))
        return jnp.where(owner < 0, 0, block)

    def plain(at, value, low_value):
        plain_ref[at] = value
        low_plain_ref[at] = low_value

    number = [lambda e, face, ref=ref: ref[e, face] for ref in (owner_ref, elem_ref, side_ref, turn_ref)]
    signs = face_tables(odd_partner(me), number, start_ref, low_start_ref, idx_ref, low_idx_ref, block_of, plain)
    for f2 in range(3):
        near = jnp.where(left, signs[2 * f2][0], signs[2 * f2 + 1][0])
        far = jnp.where(left, signs[2 * f2][1], signs[2 * f2 + 1][1])
        sign_ref[f2] = near + far
        near_ref[f2] = near
        far_ref[f2] = far
    for vp in range(6):
        block = vj_ref[vp]
        for w in range(VARS):
            spread = jnp.broadcast_to(block[:, w : w + 1], (8, 128))
            other = half_swap(spread)
            vjc_ref[(2 * vp) * VARS + w] = jnp.where(low, spread, other)
            vjc_ref[(2 * vp + 1) * VARS + w] = jnp.where(low, other, spread)
    flux_table(lambda at: fj_ref[at], fjc_ref)


def apply_inverse(inv_ref, residual, halves, stride=2):
    result = {}
    for h in range(halves):
        for v in range(VARS):
            acc = inv_ref[(v * VARS) * stride + h] * residual[0, h]
            for w in range(1, VARS):
                acc = acc + inv_ref[(v * VARS + w) * stride + h] * residual[w, h]
            result[v, h] = OMEGA * acc
    return result


def store_split(ref, row, column, first, second):
    both = jnp.concatenate([first, second], axis=0)
    high = both.astype(BF16)
    ref[row : row + 16, column : column + 128] = high
    ref[48 + row : 64 + row, column : column + 128] = (both - high.astype(F32)).astype(BF16)


def emit(state, halves, trace_ref, split_ref, face_ref, low_ref=None):
    low = rows8() < 4
    for h in range(halves):
        matrix = {}
        for vp in range(6):
            matrix[vp] = pair_turn(state[2 * vp, h], state[2 * vp + 1, h], low)
        for part in range(2):
            for vq in range(3):
                store_split(split_ref, vq * 16, (2 * h + part) * 128, matrix[2 * vq][part], matrix[2 * vq + 1][part])
    width = 256 * halves
    columns = 384 if low_ref is None else 512
    both = jnp.dot(split_ref[:, :width], trace_ref[:width, :columns], preferred_element_type=F32)
    traces = both[:48] + both[48:]
    if low_ref is not None:
        low_ref[...] = traces[:, 384:]
    for f2 in range(3):
        face_ref[f2 * 48 : f2 * 48 + 48, :] = traces[:, f2 * 128 : f2 * 128 + 128]


def to_state(matrix, halves, low):
    state = {}
    for h in range(halves):
        for vp in range(6):
            first = matrix[vp * 8 : vp * 8 + 8, 256 * h : 256 * h + 128]
            second = matrix[vp * 8 : vp * 8 + 8, 256 * h + 128 : 256 * h + 256]
            state[2 * vp, h], state[2 * vp + 1, h] = pair_turn(first, second, low)
    return state


def gather(source, start_ref, pick0, pick1):
    for face in range(6):
        target = pick1 if face % 2 else pick0
        for e in range(4):
            target[pl.ds((face // 2) * 48 + e, 12, stride=4), :] = source[pl.ds(start_ref[face * 4 + e], 12, stride=4), :]


def lifted_flux(own_ref, idx_ref, sign_ref, fjc_ref, lift_ref, pick0, pick1, jump_ref, halves):
    low = rows8() < 4
    left = lanes8() < 64
    for f2 in range(3):
        spread = {}
        for vp in range(6):
            at = f2 * 48 + vp * 8
            even = jnp.take_along_axis(pick0[at : at + 8, :], idx_ref[2 * f2], axis=1)
            odd = jnp.take_along_axis(pick1[at : at + 8, :], idx_ref[2 * f2 + 1], axis=1)
            jump = jnp.where(left, even, odd) * sign_ref[f2]
            if own_ref is not None:
                jump = own_ref[at : at + 8, :] - jump
            spread[2 * vp], spread[2 * vp + 1] = pair_turn(jump, jump, low)
        flux = []
        for vp in range(6):
            acc = fjc_ref[(f2 * 6 + vp) * VARS] * spread[0]
            for w in range(1, VARS):
                acc = acc + fjc_ref[(f2 * 6 + vp) * VARS + w] * spread[w]
            flux.append(acc)
        for vq in range(3):
            store_split(jump_ref, vq * 16, f2 * 128, flux[2 * vq], flux[2 * vq + 1])
    lifted = jnp.dot(jump_ref[...], lift_ref[:, : 256 * halves], preferred_element_type=F32)
    return to_state(lifted[:48] + lifted[48:], halves, low)


def residual_of(u_ref, base_ref, split_ref, own_ref, mine_ref, even_ref, odd_ref, start_ref, idx_ref, sign_ref,
                vjc_ref, fjc_ref, khi_ref, klo_ref, lift_ref, pool, pick0, pick1, jump_ref, halves_in, halves):
    size = mine_ref.shape[0]
    pool[0:size, :] = mine_ref[...]
    pool[size : 2 * size, :] = even_ref[...]
    if odd_ref is not None:
        pool[2 * size : 3 * size, :] = odd_ref[0:size, :]
    else:
        pool[2 * size : 3 * size, :] = mine_ref[...]
    gather(pool, start_ref, pick0, pick1)
    lifted = lifted_flux(own_ref, idx_ref, sign_ref, fjc_ref, lift_ref, pick0, pick1, jump_ref, halves)
    kin = 256 * halves_in
    kout = 256 * halves
    blended = jnp.dot(split_ref[:, :kin], khi_ref[:kin, :kout], preferred_element_type=F32)
    rest = jnp.dot(split_ref[0:48, :kin], klo_ref[:kin, :kout], preferred_element_type=F32)
    blended = to_state(blended[:48] + blended[48:] + rest, halves, rows8() < 4)
    residual = {}
    for h in range(halves):
        for v in range(VARS):
            acc = vjc_ref[v * VARS] * blended[0, h]
            for w in range(1, VARS):
                acc = acc + vjc_ref[v * VARS + w] * blended[w, h]
            residual[v, h] = base_ref[2 * v + h] - SIGMA * u_ref[2 * v + h] - acc - lifted[v, h]
    return residual


def coarse_mask():
    lane = lanes8()
    return jnp.where((((lane >> 3) & 7) < QC) & ((lane & 7) < QC), 1.0, 0.0).astype(F32)


def zero_tile():
    return jnp.zeros((8, 128), F32)


def start_all(sources, targets, sems):
    copies = [pltpu.make_async_copy(source, target, sems.at[at]) for at, (source, target) in enumerate(zip(sources, targets))]
    for copy in copies:
        copy.start()
    return copies


def first_body(me_ref, *refs):
    sources, (u_ref, split_ref, face_ref, message_ref, inv_ref, rhs_ref, trace_ref) = refs[:8], refs[8:15]
    fj_ref, numbers, sems = refs[15], refs[16:20], refs[20]
    copies = start_all(sources, (*numbers, fj_ref, inv_ref, rhs_ref, trace_ref), sems)
    for copy in copies[:5]:
        copy.wait()
    for at in range(36):
        row = FLUX_ROW + 8 * (at // 8)
        column = 16 * (at % 8)
        message_ref[row : row + 8, column : column + 12] = fj_ref[at]
    for at in range(4):
        row = NUMBER_ROW + 4 * at
        message_ref[row : row + 4, 0:6] = numbers[at][...].astype(F32)
    copies[5].wait()
    copies[6].wait()
    state = apply_inverse(inv_ref, {(v, h): rhs_ref[2 * v + h] for v in range(VARS) for h in range(2)}, 2)
    for v in range(VARS):
        for h in range(2):
            u_ref[2 * v + h] = state[v, h]
    lane = lanes8()
    place = ((lane >> 4) & 1) * 64 + ((lane >> 2) & 3) * 8 + (lane & 3)
    for at in range(36):
        tiles = [jnp.take_along_axis(inv_ref[2 * (4 * at + part)], place, axis=1) for part in range(4)]
        packed = jnp.where(lane < 64, jnp.where(lane < 32, tiles[0], tiles[1]), jnp.where(lane < 96, tiles[2], tiles[3]))
        message_ref[144 + 8 * at : 152 + 8 * at, :] = packed
    copies[7].wait()
    emit(state, 2, trace_ref, split_ref, face_ref)
    message_ref[0:144, :] = face_ref[...]


def ghost_prepare_body(me_ref, far_ref, start_ref, idx_ref, sign_ref, fjc_ref, inv_ref,
                       fine_start_ref, fine_idx_ref, number_ref, sems):
    copy = pltpu.make_async_copy(far_ref.at[pl.ds(NUMBER_ROW, 16)], number_ref, sems.at[0])
    copy.start()
    flux_table(
        lambda at: far_ref[FLUX_ROW + 8 * (at // 8) : FLUX_ROW + 8 * (at // 8) + 8, 16 * (at % 8) : 16 * (at % 8) + 12],
        fjc_ref,
    )
    lane = lanes8()
    place = ((lane >> 6) & 1) * 16 + ((lane >> 3) & 3) * 4 + (lane & 3)
    for at in range(36):
        packed = far_ref[144 + 8 * at : 152 + 8 * at, :]
        for part in range(4):
            inv_ref[4 * at + part] = jnp.take_along_axis(packed, place + 32 * part, axis=1)
    copy.wait()
    left = lanes8() < 64
    number = [lambda e, face, at=at: number_ref[4 * at + e, face].astype(jnp.int32) for at in range(4)]
    signs = face_tables(
        me_ref[0], number, fine_start_ref, start_ref, fine_idx_ref, idx_ref, lambda owner: 0, lambda *values: None
    )
    for f2 in range(3):
        sign_ref[f2] = jnp.where(left, signs[2 * f2][1], signs[2 * f2 + 1][1])


def prepare_body(me_ref, *refs):
    sources, tables, (khi_ref, klo_ref, lift_ref) = refs[:8], refs[8:19], refs[19:22]
    owner_ref, elem_ref, side_ref, turn_ref, vj_ref, fj_ref, stiff_ref, sems = refs[22:]
    copies = start_all(sources, (owner_ref, elem_ref, side_ref, turn_ref, vj_ref, fj_ref, stiff_ref, lift_ref), sems)
    for copy in copies[:6]:
        copy.wait()
    prepare_tables(me_ref[0], owner_ref, elem_ref, side_ref, turn_ref, vj_ref, fj_ref, *tables)
    copies[6].wait()
    stiff = stiff_ref[...]
    high = stiff.astype(BF16)
    khi_ref[...] = high
    klo_ref[...] = (stiff - high.astype(F32)).astype(BF16)
    copies[7].wait()


def fine_body(inv_ref, trace_ref, u_ref, *rest):
    fine_step(inv_ref, trace_ref, u_ref, rest[:14], *rest[14:17], None, rest[17:])


def fine_low_body(inv_ref, trace_ref, u_ref, *rest):
    fine_step(inv_ref, trace_ref, u_ref, rest[:14], *rest[14:18], rest[18:])


def fine_step(inv_ref, trace_ref, u_ref, shared, out_ref, split_ref, face_ref, low_ref, scratch):
    residual = residual_of(u_ref, *shared, *scratch, 2, 2)
    state = apply_inverse(inv_ref, residual, 2)
    for v in range(VARS):
        for h in range(2):
            state[v, h] = state[v, h] + u_ref[2 * v + h]
            out_ref[2 * v + h] = state[v, h]
    emit(state, 2, trace_ref, split_ref, face_ref, low_ref)


def last_body(inv_ref, u_ref, *rest):
    shared, out_hbm, scratch, out_ref, sems = rest[:14], rest[14], rest[15:19], rest[19], rest[20]
    residual = residual_of(u_ref, *shared, *scratch, 2, 2)
    copies = []
    for part in range(3):
        for v in range(4 * part, 4 * part + 4):
            for h in range(2):
                acc = inv_ref[(v * VARS) * 2 + h] * residual[0, h]
                for w in range(1, VARS):
                    acc = acc + inv_ref[(v * VARS + w) * 2 + h] * residual[w, h]
                out_ref[2 * v + h] = OMEGA * acc + u_ref[2 * v + h]
        piece = pl.ds(8 * part, 8)
        copies.append(pltpu.make_async_copy(out_ref.at[piece], out_hbm.at[piece], sems.at[part]))
        copies[-1].start()
    for copy in copies:
        copy.wait()


def local_step(coarse, u_ref, base_ref, split_ref, own_ref, mine_ref, even_ref, *rest):
    tables, payload_ref, scratch = rest[:8], rest[8], rest[9:]
    halves = 1 if coarse else 2
    residual = residual_of(u_ref, base_ref, split_ref, own_ref, mine_ref, even_ref, None, *tables, *scratch, 2, halves)
    size = mine_ref.shape[0]
    payload_ref[0:size, :] = mine_ref[...]
    mask = coarse_mask() if coarse else None
    for v in range(VARS):
        for h in range(halves):
            at = size + 8 * (halves * v + h)
            payload_ref[at : at + 8, :] = residual[v, h] * mask if coarse else residual[v, h]


def local_low_body(*refs):
    local_step(True, *refs)


def joined(base_ref, source_ref, halves, start_ref, idx_ref, sign_ref, fjc_ref, lift_ref, pick0, pick1, jump_ref):
    gather(source_ref, start_ref, pick0, pick1)
    lifted = lifted_flux(None, idx_ref, sign_ref, fjc_ref, lift_ref, pick0, pick1, jump_ref, halves)
    size = base_ref.shape[0] - 96 * halves
    mask = coarse_mask()
    residual = {}
    for v in range(VARS):
        for h in range(halves):
            at = size + 8 * (halves * v + h)
            flux = lifted[v, h] * mask if halves == 1 else lifted[v, h]
            residual[v, h] = base_ref[at : at + 8, :] + flux
    return residual


def own_low_body(inv_ref, trace_ref, mine_ref, far_ref, *rest):
    tables, (low_ref, out_ref, split_ref, face_ref, sent_ref), scratch = rest[:5], rest[5:10], rest[10:]
    residual = joined(mine_ref, far_ref, 1, *tables, *scratch)
    state = apply_inverse(inv_ref, residual, 1)
    for v in range(VARS):
        low_ref[2 * v] = residual[v, 0]
        low_ref[2 * v + 1] = zero_tile()
        out_ref[2 * v] = state[v, 0]
        out_ref[2 * v + 1] = zero_tile()
    emit(state, 1, trace_ref, split_ref, face_ref, sent_ref)


def ghost_low_body(inv_ref, trace_ref, mine_ref, far_ref, *rest):
    tables, sent_ref, scratch = rest[:5], rest[5], rest[6:]
    residual = joined(far_ref, mine_ref, 1, *tables, *scratch[:3])
    emit(apply_inverse(inv_ref, residual, 1, stride=1), 1, trace_ref, scratch[3], scratch[4], sent_ref)


def coarse_body(inv_ref, trace_ref, fine_ref, u_ref, *rest):
    shared, (out_ref, split_ref, face_ref), scratch = rest[:14], rest[14:17], rest[17:]
    residual = residual_of(u_ref, *shared, *scratch, 1, 1)
    mask = coarse_mask()
    residual = {key: tile * mask for key, tile in residual.items()}
    state = apply_inverse(inv_ref, residual, 1)
    for v in range(VARS):
        state[v, 0] = state[v, 0] + u_ref[2 * v] + fine_ref[2 * v]
        state[v, 1] = fine_ref[2 * v + 1]
        out_ref[2 * v] = state[v, 0]
        out_ref[2 * v + 1] = state[v, 1]
    emit(state, 2, trace_ref, split_ref, face_ref)


STATE = VMEM((24, 8, 128), F32)
SPLIT = VMEM((96, 512), BF16)
FACES = VMEM((144, 128), F32)
LOW_FACES = VMEM((48, 128), F32)


def in_vmem(value):
    return pltpu.with_memory_space_constraint(value, VMEM)


def in_hbm(value):
    return pltpu.with_memory_space_constraint(value, pltpu.HBM)


def call(body, outs, args, scratch=(), smem=(), smem_outs=(), far=False, far_out=False):
    spec = pl.BlockSpec(memory_space=VMEM)
    source = pl.BlockSpec(memory_space=pl.ANY) if far else spec
    target = pl.BlockSpec(memory_space=pl.ANY) if far_out else spec
    scalar = pl.BlockSpec(memory_space=pltpu.SMEM)
    return pl.pallas_call(
        body,
        out_shape=list(outs),
        in_specs=[scalar if at in smem else source for at in range(len(args))],
        out_specs=[scalar if at in smem_outs else target for at in range(len(outs))],
        scratch_shapes=list(scratch),
        compiler_params=pltpu.CompilerParams(vmem_limit_bytes=6 * 1024 * 1024),
    )(*args)


def odd_swap(value):
    count = lax.axis_size("dom")
    route = []
    for at in range(1, count - 1, 2):
        route += [(at, at + 1), (at + 1, at)]
    return lax.ppermute(value, "dom", route)


def even_swap(value):
    return in_vmem(lax.ppermute(value, "dom", [(at, at ^ 1) for at in range(lax.axis_size("dom"))]))


def cycle(rhs, stiffness, vol_jac, face_jac, block_inv, face_owner, face_elem, face_side, face_turn):
    me = lax.axis_index("dom").astype(jnp.int32).reshape(1)
    rhs_state = rhs.reshape(4, 12, 4, 128).transpose(1, 2, 0, 3).reshape(24, 8, 128)
    inverse = block_inv.reshape(4, 12, 12, 4, 128).transpose(1, 2, 3, 0, 4).reshape(288, 8, 128)
    vj = vol_jac.transpose(1, 0, 2).reshape(6, 8, 12)
    fj = face_jac.transpose(1, 2, 0, 3).reshape(36, 8, 12)
    trace = jnp.asarray(np.concatenate([trace_matrix(), low_trace_matrix()], 1), BF16)
    lift = jnp.asarray(lift_matrix(), BF16)
    numbers = (face_owner, face_elem, face_side, face_turn)
    integers = pltpu.SMEM((24,), jnp.int32)
    indices = VMEM((6, 8, 128), jnp.int32)
    signs = VMEM((3, 8, 128), F32)
    u, split, faces, message, inverse, rhs_state, trace = call(
        first_body,
        (
            STATE,
            SPLIT,
            FACES,
            VMEM((MESSAGE_ROWS, 128), F32),
            VMEM((288, 8, 128), F32),
            STATE,
            VMEM(trace.shape, BF16),
        ),
        (me, *(in_hbm(load) for load in (*numbers, fj, inverse, rhs_state, trace))),
        (VMEM((36, 8, 12), F32), *(VMEM((4, 6), jnp.int32) for _ in range(4)), pltpu.SemaphoreType.DMA((8,))),
        smem=(0,),
        far=True,
    )
    far_message = in_vmem(odd_swap(message))
    even = even_swap(faces)
    loads = (*numbers, vj, fj, stiffness, lift)
    start, idx, sign, low_start, low_idx, near, far, _, low_plain, vjc, fjc, khi, klo, lift = call(
        prepare_body,
        (
            integers,
            indices,
            signs,
            integers,
            indices,
            signs,
            signs,
            integers,
            integers,
            VMEM((144, 8, 128), F32),
            VMEM((216, 8, 128), F32),
            VMEM((512, 512), BF16),
            VMEM((512, 512), BF16),
            VMEM((384, 512), BF16),
        ),
        (me, *(in_hbm(load) for load in loads)),
        (
            *(pltpu.SMEM((4, 6), jnp.int32) for _ in range(4)),
            VMEM((6, 8, 12), F32),
            VMEM((36, 8, 12), F32),
            VMEM((512, 512), F32),
            pltpu.SemaphoreType.DMA((8,)),
        ),
        smem=(0,),
        smem_outs=(0, 3, 7, 8),
        far=True,
    )
    volume = (vjc, fjc, khi, klo, lift)
    picks = (FACES, FACES, VMEM((96, 384), BF16))
    pool = (VMEM((432, 128), F32), *picks)

    fine_two, split, faces, sent = call(
        fine_low_body,
        (STATE, SPLIT, FACES, LOW_FACES),
        (inverse, trace, u, rhs_state, split, faces, faces, even, far_message, start, idx, sign, *volume),
        pool,
        smem=(9,),
    )
    even = even_swap(sent)
    (payload,) = call(
        local_low_body,
        (FACES,),
        (fine_two, rhs_state, split, faces, sent, even, low_start, low_idx, near, *volume),
        pool,
        smem=(6,),
    )
    far_payload = in_vmem(odd_swap(payload))
    ghost_start, ghost_idx, ghost_sign, ghost_fjc, ghost_inverse = call(
        ghost_prepare_body,
        (integers, indices, signs, VMEM((216, 8, 128), F32), VMEM((144, 8, 128), F32)),
        (me, far_message),
        (
            pltpu.SMEM((24,), jnp.int32),
            VMEM((6, 8, 128), jnp.int32),
            pltpu.SMEM((16, 128), F32),
            pltpu.SemaphoreType.DMA((1,)),
        ),
        smem=(0,),
        smem_outs=(0,),
    )
    low_rhs, coarse, split, faces, sent = call(
        own_low_body,
        (STATE, STATE, SPLIT, FACES, LOW_FACES),
        (inverse, trace, payload, far_payload, low_plain, low_idx, far, fjc, lift),
        picks,
        smem=(4,),
    )
    even = even_swap(sent)
    (odd,) = call(
        ghost_low_body,
        (LOW_FACES,),
        (ghost_inverse, trace, payload, far_payload, ghost_start, ghost_idx, ghost_sign, ghost_fjc, lift),
        (*picks, SPLIT, FACES),
        smem=(4,),
    )
    u, split, faces = call(
        coarse_body,
        (STATE, SPLIT, FACES),
        (inverse, trace, fine_two, coarse, low_rhs, split, faces, sent, even, odd, low_start, low_idx, sign, *volume),
        pool,
        smem=(10,),
    )
    odd = in_vmem(odd_swap(faces))
    even = even_swap(faces)
    u, split, faces = call(
        fine_body,
        (STATE, SPLIT, FACES),
        (inverse, trace, u, rhs_state, split, faces, faces, even, odd, start, idx, sign, *volume),
        pool,
        smem=(9,),
    )
    odd = in_vmem(odd_swap(faces))
    even = even_swap(faces)
    (u,) = call(
        last_body,
        (jax.ShapeDtypeStruct((24, 8, 128), F32),),
        (inverse, u, rhs_state, split, faces, faces, even, odd, start, idx, sign, *volume),
        (*pool, STATE, pltpu.SemaphoreType.DMA((3,))),
        smem=(8,),
        far_out=True,
    )
    return u.reshape(12, 4, 4, 128).transpose(2, 0, 1, 3).reshape(4, 12, 512)


def solution(mesh):
    dom = P("dom")
    return jax.shard_map(
        cycle,
        mesh=mesh,
        in_specs=(dom, P(), dom, dom, dom, dom, dom, dom, dom),
        out_specs=dom,
        check_vma=False,
    )
```

```python
import jax
import jax.numpy as jnp
import numpy as np
from jax import lax
from jax.experimental import pallas as pl
from jax.experimental.pallas import tpu as pltpu
from jax.sharding import PartitionSpec as P


QF = 8
QC = 4
VARS = 12
FLUX_ROW = 144 + 288
NUMBER_ROW = FLUX_ROW + 40
MESSAGE_ROWS = NUMBER_ROW + 16
SIGMA = 2.0
OMEGA = 0.7
F32 = jnp.float32
BF16 = jnp.bfloat16
VMEM = pltpu.VMEM


def trace_matrix():
    matrix = np.zeros((512, 384), np.float32)
    for i in range(QF):
        for j in range(QF):
            for k in range(QF):
                mode = (i * QF + j) * QF + k
                triple = (i, j, k)
                for face in range(6):
                    normal = triple[face // 2]
                    a, b = [triple[place] for place in range(3) if place != face // 2]
                    matrix[mode, face * 64 + a * 8 + b] = (-1.0) ** normal if face % 2 == 0 else 1.0
    return matrix


def low_trace_matrix():
    places = [face * 64 + a * 8 + b for face in range(6) for a in range(QC) for b in range(QC)]
    return np.pad(trace_matrix()[:, places], ((0, 0), (0, 32)))


def lift_matrix():
    degrees = np.stack(np.meshgrid(*[np.arange(QF)] * 3, indexing="ij"), -1).reshape(512, 3)
    scale = np.stack([(2.0 * degrees[:, face // 2] + 1.0) / 16.0 for face in range(6)], -1)
    return (trace_matrix().reshape(512, 6, 64) * scale[:, :, None]).reshape(512, 384).T


def rows8():
    return lax.broadcasted_iota(jnp.int32, (8, 128), 0)


def lanes8():
    return lax.broadcasted_iota(jnp.int32, (8, 128), 1)


def half_swap(tile):
    return pltpu.roll(tile, 4, axis=0)


def pair_turn(first, second, low):
    return jnp.where(low, first, half_swap(second)), jnp.where(low, half_swap(first), second)


def face_tables(other, number, start_ref, low_start_ref, idx_ref, low_idx_ref, block_of, masks,
                short_start_ref, short_idx_ref):
    owner_of, elem_of, side_of, turn_of = number
    rows = rows8()
    lane = lanes8()
    element = rows & 3
    a = (lane >> 3) & 7
    b = lane & 7
    count = jnp.int32(0)
    signs = []
    for face in range(6):
        sides = jnp.zeros((8, 128), jnp.int32)
        turns = jnp.zeros((8, 128), jnp.int32)
        here_far = jnp.zeros((8, 128), jnp.int32)
        here_near = jnp.zeros((8, 128), jnp.int32)
        parities = jnp.zeros((8, 128), jnp.int32)
        for e in range(4):
            owner = owner_of(e, face)
            side = side_of(e, face)
            elem = elem_of(e, face)
            block = block_of(owner)
            start_ref[face * 4 + e] = block * 144 + (side >> 1) * 48 + elem
            low_start_ref[face * 4 + e] = block * 48 + elem
            masks(face * 4 + e, (side >> 1) * 48 + elem, elem)
            here = element == e
            turns = jnp.where(here, turn_of(e, face), turns)
            sides = jnp.where(here, side, sides)
            far = jnp.where((owner >= 0) & (owner == other), 1, 0)
            short_start_ref[face * 4 + e] = jnp.where(far == 1, 288 + (count >> 1), block * 144 + (side >> 1) * 48 + elem)
            parities = jnp.where(here, jnp.where(far == 1, count & 1, side & 1), parities)
            count = count + far
            here_far = jnp.where(here, far, here_far)
            here_near = jnp.where(here, jnp.where(owner >= 0, 1, 0) - far, here_near)
        swap = (turns & 1) == 1
        place = jnp.where(swap, b * 8 + a, a * 8 + b)
        idx_ref[face] = (sides & 1) * 64 + place
        short_idx_ref[face] = parities * 64 + place
        low_idx_ref[face] = sides * 16 + jnp.where(swap, (b & 3) * 4 + (a & 3), (a & 3) * 4 + (b & 3))
        flips = 1 - 2 * ((((turns >> 1) & a) + ((turns >> 2) & b)) & 1)
        signs.append(((here_near * flips).astype(F32), (here_far * flips).astype(F32)))
    return signs


def flux_table(block_of, fjc_ref):
    left = lanes8() < 64
    for f2 in range(3):
        for vp in range(6):
            even = block_of(2 * f2 * 6 + vp)
            odd = block_of((2 * f2 + 1) * 6 + vp)
            for w in range(VARS):
                fjc_ref[(f2 * 6 + vp) * VARS + w] = jnp.where(
                    left,
                    jnp.broadcast_to(even[:, w : w + 1], (8, 128)),
                    jnp.broadcast_to(odd[:, w : w + 1], (8, 128)),
                )


def odd_partner(me):
    return me - 1 + 2 * (me & 1)


def prepare_tables(me, owner_ref, elem_ref, side_ref, turn_ref, vj_ref, fj_ref, start_ref, idx_ref, sign_ref,
                   low_start_ref, low_idx_ref, near_ref, far_ref, low_plain_ref, short_start_ref, short_idx_ref,
                   vjc_ref, fjc_ref):
    left = lanes8() < 64
    low = rows8() < 4

    def block_of(owner):
        block = jnp.where(owner == me, 0, jnp.where(owner == (me ^ 1), 1, 2))
        return jnp.where(owner < 0, 0, block)

    def plain(at, value, low_value):
        low_plain_ref[at] = low_value

    number = [lambda e, face, ref=ref: ref[e, face] for ref in (owner_ref, elem_ref, side_ref, turn_ref)]
    signs = face_tables(odd_partner(me), number, start_ref, low_start_ref, idx_ref, low_idx_ref, block_of, plain,
                        short_start_ref, short_idx_ref)
    for f2 in range(3):
        near = jnp.where(left, signs[2 * f2][0], signs[2 * f2 + 1][0])
        far = jnp.where(left, signs[2 * f2][1], signs[2 * f2 + 1][1])
        sign_ref[f2] = near + far
        near_ref[f2] = near
        far_ref[f2] = far
    for vp in range(6):
        block = vj_ref[vp]
        for w in range(VARS):
            spread = jnp.broadcast_to(block[:, w : w + 1], (8, 128))
            other = half_swap(spread)
            vjc_ref[(2 * vp) * VARS + w] = jnp.where(low, spread, other)
            vjc_ref[(2 * vp + 1) * VARS + w] = jnp.where(low, other, spread)
    flux_table(lambda at: fj_ref[at], fjc_ref)


def apply_inverse(inv_ref, residual, halves, stride=2):
    result = {}
    for h in range(halves):
        for v in range(VARS):
            acc = inv_ref[(v * VARS) * stride + h] * residual[0, h]
            for w in range(1, VARS):
                acc = acc + inv_ref[(v * VARS + w) * stride + h] * residual[w, h]
            result[v, h] = OMEGA * acc
    return result


def store_split(ref, row, column, first, second):
    both = jnp.concatenate([first, second], axis=0)
    high = both.astype(BF16)
    ref[row : row + 16, column : column + 128] = high
    ref[48 + row : 64 + row, column : column + 128] = (both - high.astype(F32)).astype(BF16)


def emit(state, halves, trace_ref, split_ref, face_ref, low_ref=None):
    low = rows8() < 4
    for h in range(halves):
        matrix = {}
        for vp in range(6):
            matrix[vp] = pair_turn(state[2 * vp, h], state[2 * vp + 1, h], low)
        for part in range(2):
            for vq in range(3):
                store_split(split_ref, vq * 16, (2 * h + part) * 128, matrix[2 * vq][part], matrix[2 * vq + 1][part])
    width = 256 * halves
    columns = 384 if low_ref is None else 512
    both = jnp.dot(split_ref[:, :width], trace_ref[:width, :columns], preferred_element_type=F32)
    traces = both[:48] + both[48:]
    if low_ref is not None:
        low_ref[...] = traces[:, 384:]
    for f2 in range(3):
        face_ref[f2 * 48 : f2 * 48 + 48, :] = traces[:, f2 * 128 : f2 * 128 + 128]


def answer(face_ref, ask_ref, ask_idx_ref, pick0, pick1, short_ref):
    left = lanes8() < 64
    for at in range(8):
        target = pick1 if at % 2 else pick0
        target[pl.ds(at // 2, 12, stride=4), :] = face_ref[pl.ds(ask_ref[at], 12, stride=4), :]
    for vp in range(6):
        row = 8 * vp
        even = jnp.take_along_axis(pick0[row : row + 8, :], ask_idx_ref[0], axis=1)
        odd = jnp.take_along_axis(pick1[row : row + 8, :], ask_idx_ref[1], axis=1)
        short_ref[row : row + 8, :] = jnp.where(left, even, odd)


def to_state(matrix, halves, low):
    state = {}
    for h in range(halves):
        for vp in range(6):
            first = matrix[vp * 8 : vp * 8 + 8, 256 * h : 256 * h + 128]
            second = matrix[vp * 8 : vp * 8 + 8, 256 * h + 128 : 256 * h + 256]
            state[2 * vp, h], state[2 * vp + 1, h] = pair_turn(first, second, low)
    return state


def gather(source, start_ref, pick0, pick1):
    for face in range(6):
        target = pick1 if face % 2 else pick0
        for e in range(4):
            target[pl.ds((face // 2) * 48 + e, 12, stride=4), :] = source[pl.ds(start_ref[face * 4 + e], 12, stride=4), :]


def lifted_flux(own_ref, idx_ref, sign_ref, fjc_ref, lift_ref, pick0, pick1, jump_ref, halves):
    low = rows8() < 4
    left = lanes8() < 64
    for f2 in range(3):
        spread = {}
        for vp in range(6):
            at = f2 * 48 + vp * 8
            even = jnp.take_along_axis(pick0[at : at + 8, :], idx_ref[2 * f2], axis=1)
            odd = jnp.take_along_axis(pick1[at : at + 8, :], idx_ref[2 * f2 + 1], axis=1)
            jump = jnp.where(left, even, odd) * sign_ref[f2]
            if own_ref is not None:
                jump = own_ref[at : at + 8, :] - jump
            spread[2 * vp], spread[2 * vp + 1] = pair_turn(jump, jump, low)
        flux = []
        for vp in range(6):
            acc = fjc_ref[(f2 * 6 + vp) * VARS] * spread[0]
            for w in range(1, VARS):
                acc = acc + fjc_ref[(f2 * 6 + vp) * VARS + w] * spread[w]
            flux.append(acc)
        for vq in range(3):
            store_split(jump_ref, vq * 16, f2 * 128, flux[2 * vq], flux[2 * vq + 1])
    lifted = jnp.dot(jump_ref[...], lift_ref[:, : 256 * halves], preferred_element_type=F32)
    return to_state(lifted[:48] + lifted[48:], halves, low)


def residual_of(u_ref, base_ref, split_ref, own_ref, mine_ref, even_ref, odd_ref, start_ref, idx_ref, sign_ref,
                vjc_ref, fjc_ref, khi_ref, klo_ref, lift_ref, pool, pick0, pick1, jump_ref, halves_in, halves):
    kin = 256 * halves_in
    kout = 256 * halves
    blended = jnp.dot(split_ref[:, :kin], khi_ref[:kin, :kout], preferred_element_type=F32)
    rest = jnp.dot(split_ref[0:48, :kin], klo_ref[:kin, :kout], preferred_element_type=F32)
    size = mine_ref.shape[0]
    pool[0:size, :] = mine_ref[...]
    pool[size : 2 * size, :] = even_ref[...]
    if odd_ref is not None:
        count = min(size, odd_ref.shape[0])
        pool[2 * size : 2 * size + count, :] = odd_ref[0:count, :]
    else:
        pool[2 * size : 3 * size, :] = mine_ref[...]
    gather(pool, start_ref, pick0, pick1)
    blended = to_state(blended[:48] + blended[48:] + rest, halves, rows8() < 4)
    residual = {}
    for h in range(halves):
        for v in range(VARS):
            acc = vjc_ref[v * VARS] * blended[0, h]
            for w in range(1, VARS):
                acc = acc + vjc_ref[v * VARS + w] * blended[w, h]
            residual[v, h] = base_ref[2 * v + h] - SIGMA * u_ref[2 * v + h] - acc
    lifted = lifted_flux(own_ref, idx_ref, sign_ref, fjc_ref, lift_ref, pick0, pick1, jump_ref, halves)
    return {key: tile - lifted[key] for key, tile in residual.items()}


def coarse_mask():
    lane = lanes8()
    return jnp.where((((lane >> 3) & 7) < QC) & ((lane & 7) < QC), 1.0, 0.0).astype(F32)


def zero_tile():
    return jnp.zeros((8, 128), F32)


def start_all(sources, targets, sems):
    copies = [pltpu.make_async_copy(source, target, sems.at[at]) for at, (source, target) in enumerate(zip(sources, targets))]
    for copy in copies:
        copy.start()
    return copies


def first_body(me_ref, *refs):
    sources, (u_ref, split_ref, face_ref, message_ref, inv_ref, rhs_ref, trace_ref) = refs[:8], refs[8:15]
    fj_ref, numbers, sems = refs[15], refs[16:20], refs[20]
    copies = start_all(sources, (*numbers, fj_ref, inv_ref, rhs_ref, trace_ref), sems)
    for copy in copies[:5]:
        copy.wait()
    for at in range(36):
        row = FLUX_ROW + 8 * (at // 8)
        column = 16 * (at % 8)
        message_ref[row : row + 8, column : column + 12] = fj_ref[at]
    for at in range(4):
        row = NUMBER_ROW + 4 * at
        message_ref[row : row + 4, 0:6] = numbers[at][...].astype(F32)
    copies[5].wait()
    copies[6].wait()
    state = apply_inverse(inv_ref, {(v, h): rhs_ref[2 * v + h] for v in range(VARS) for h in range(2)}, 2)
    for v in range(VARS):
        for h in range(2):
            u_ref[2 * v + h] = state[v, h]
    copies[7].wait()
    emit(state, 2, trace_ref, split_ref, face_ref)
    lane = lanes8()
    place = ((lane >> 4) & 1) * 64 + ((lane >> 2) & 3) * 8 + (lane & 3)
    for at in range(36):
        tiles = [jnp.take_along_axis(inv_ref[2 * (4 * at + part)], place, axis=1) for part in range(4)]
        packed = jnp.where(lane < 64, jnp.where(lane < 32, tiles[0], tiles[1]), jnp.where(lane < 96, tiles[2], tiles[3]))
        message_ref[144 + 8 * at : 152 + 8 * at, :] = packed
    message_ref[0:144, :] = face_ref[...]


def ghost_prepare_body(me_ref, far_ref, start_ref, idx_ref, sign_ref, fjc_ref, inv_ref, ask_ref, ask_idx_ref,
                       fine_start_ref, fine_idx_ref, parity_ref, number_ref, sems):
    copy = pltpu.make_async_copy(far_ref.at[pl.ds(NUMBER_ROW, 16)], number_ref, sems.at[0])
    copy.start()
    flux_table(
        lambda at: far_ref[FLUX_ROW + 8 * (at // 8) : FLUX_ROW + 8 * (at // 8) + 8, 16 * (at % 8) : 16 * (at % 8) + 12],
        fjc_ref,
    )
    lane = lanes8()
    place = ((lane >> 6) & 1) * 16 + ((lane >> 3) & 3) * 4 + (lane & 3)
    for at in range(36):
        packed = far_ref[144 + 8 * at : 152 + 8 * at, :]
        for part in range(4):
            inv_ref[4 * at + part] = jnp.take_along_axis(packed, place + 32 * part, axis=1)
    copy.wait()
    left = lanes8() < 64
    number = [lambda e, face, at=at: number_ref[4 * at + e, face].astype(jnp.int32) for at in range(4)]
    signs = face_tables(
        me_ref[0], number, fine_start_ref, start_ref, fine_idx_ref, idx_ref, lambda owner: 0, lambda *values: None,
        fine_start_ref, fine_idx_ref,
    )
    for at in range(32):
        ask_ref[at] = 0
        parity_ref[at] = 0
    count = jnp.int32(0)
    for face in range(6):
        for e in range(4):
            side = number[2](e, face)
            ask_ref[count] = (side >> 1) * 48 + number[1](e, face)
            parity_ref[count] = side & 1
            count = count + jnp.where(number[0](e, face) == me_ref[0], 1, 0)
    for half in range(2):
        parity = jnp.zeros((8, 128), jnp.int32)
        for quarter in range(4):
            parity = jnp.where((rows8() & 3) == quarter, parity_ref[2 * quarter + half], parity)
        ask_idx_ref[half] = parity * 64 + (lane & 63)
    for f2 in range(3):
        sign_ref[f2] = jnp.where(left, signs[2 * f2][1], signs[2 * f2 + 1][1])


def prepare_body(me_ref, *refs):
    sources, tables, (khi_ref, klo_ref, lift_ref) = refs[:8], refs[8:20], refs[20:23]
    owner_ref, elem_ref, side_ref, turn_ref, vj_ref, fj_ref, stiff_ref, sems = refs[23:]
    copies = start_all(sources, (owner_ref, elem_ref, side_ref, turn_ref, vj_ref, fj_ref, stiff_ref, lift_ref), sems)
    for copy in copies[:6]:
        copy.wait()
    prepare_tables(me_ref[0], owner_ref, elem_ref, side_ref, turn_ref, vj_ref, fj_ref, *tables)
    copies[6].wait()
    stiff = stiff_ref[...]
    high = stiff.astype(BF16)
    khi_ref[...] = high
    klo_ref[...] = (stiff - high.astype(F32)).astype(BF16)
    copies[7].wait()


def fine_body(inv_ref, trace_ref, u_ref, *rest):
    fine_step(inv_ref, trace_ref, u_ref, rest[:14], *rest[16:19], None, rest[20:])
    answer(rest[18], *rest[14:16], *rest[21:23], rest[19])


def fine_low_body(inv_ref, trace_ref, u_ref, *rest):
    fine_step(inv_ref, trace_ref, u_ref, rest[:14], *rest[14:18], rest[18:])


def fine_step(inv_ref, trace_ref, u_ref, shared, out_ref, split_ref, face_ref, low_ref, scratch):
    residual = residual_of(u_ref, *shared, *scratch, 2, 2)
    state = apply_inverse(inv_ref, residual, 2)
    for v in range(VARS):
        for h in range(2):
            state[v, h] = state[v, h] + u_ref[2 * v + h]
            out_ref[2 * v + h] = state[v, h]
    emit(state, 2, trace_ref, split_ref, face_ref, low_ref)


def last_body(inv_ref, u_ref, *rest):
    shared, out_hbm, scratch, out_ref, sems = rest[:14], rest[14], rest[15:19], rest[19], rest[20]
    residual = residual_of(u_ref, *shared, *scratch, 2, 2)
    copies = []
    for part in range(3):
        for v in range(4 * part, 4 * part + 4):
            for h in range(2):
                acc = inv_ref[(v * VARS) * 2 + h] * residual[0, h]
                for w in range(1, VARS):
                    acc = acc + inv_ref[(v * VARS + w) * 2 + h] * residual[w, h]
                out_ref[2 * v + h] = OMEGA * acc + u_ref[2 * v + h]
        piece = pl.ds(8 * part, 8)
        copies.append(pltpu.make_async_copy(out_ref.at[piece], out_hbm.at[piece], sems.at[part]))
        copies[-1].start()
    for copy in copies:
        copy.wait()


def local_step(coarse, u_ref, base_ref, split_ref, own_ref, mine_ref, even_ref, *rest):
    tables, payload_ref, scratch = rest[:8], rest[8], rest[9:]
    halves = 1 if coarse else 2
    residual = residual_of(u_ref, base_ref, split_ref, own_ref, mine_ref, even_ref, None, *tables, *scratch, 2, halves)
    size = mine_ref.shape[0]
    payload_ref[0:size, :] = mine_ref[...]
    mask = coarse_mask() if coarse else None
    for v in range(VARS):
        for h in range(halves):
            at = size + 8 * (halves * v + h)
            payload_ref[at : at + 8, :] = residual[v, h] * mask if coarse else residual[v, h]


def local_low_body(*refs):
    local_step(True, *refs)


def joined(base_ref, source_ref, halves, start_ref, idx_ref, sign_ref, fjc_ref, lift_ref, pick0, pick1, jump_ref):
    gather(source_ref, start_ref, pick0, pick1)
    lifted = lifted_flux(None, idx_ref, sign_ref, fjc_ref, lift_ref, pick0, pick1, jump_ref, halves)
    size = base_ref.shape[0] - 96 * halves
    mask = coarse_mask()
    residual = {}
    for v in range(VARS):
        for h in range(halves):
            at = size + 8 * (halves * v + h)
            flux = lifted[v, h] * mask if halves == 1 else lifted[v, h]
            residual[v, h] = base_ref[at : at + 8, :] + flux
    return residual


def own_low_body(inv_ref, trace_ref, mine_ref, far_ref, *rest):
    tables, (low_ref, out_ref, split_ref, face_ref, sent_ref), scratch = rest[:5], rest[5:10], rest[10:]
    residual = joined(mine_ref, far_ref, 1, *tables, *scratch)
    state = apply_inverse(inv_ref, residual, 1)
    for v in range(VARS):
        low_ref[2 * v] = residual[v, 0]
        low_ref[2 * v + 1] = zero_tile()
        out_ref[2 * v] = state[v, 0]
        out_ref[2 * v + 1] = zero_tile()
    emit(state, 1, trace_ref, split_ref, face_ref, sent_ref)


def ghost_low_body(inv_ref, trace_ref, mine_ref, far_ref, *rest):
    tables, sent_ref, scratch = rest[:5], rest[5], rest[6:]
    residual = joined(far_ref, mine_ref, 1, *tables, *scratch[:3])
    emit(apply_inverse(inv_ref, residual, 1, stride=1), 1, trace_ref, scratch[3], scratch[4], sent_ref)


def coarse_body(inv_ref, trace_ref, fine_ref, u_ref, *rest):
    shared, (out_ref, split_ref, face_ref), scratch = rest[:14], rest[16:19], rest[20:]
    residual = residual_of(u_ref, *shared, *scratch, 1, 1)
    mask = coarse_mask()
    residual = {key: tile * mask for key, tile in residual.items()}
    state = apply_inverse(inv_ref, residual, 1)
    for v in range(VARS):
        state[v, 0] = state[v, 0] + u_ref[2 * v] + fine_ref[2 * v]
        state[v, 1] = fine_ref[2 * v + 1]
        out_ref[2 * v] = state[v, 0]
        out_ref[2 * v + 1] = state[v, 1]
    emit(state, 2, trace_ref, split_ref, face_ref)
    answer(face_ref, *rest[14:16], *scratch[1:3], rest[19])


STATE = VMEM((24, 8, 128), F32)
SPLIT = VMEM((96, 512), BF16)
FACES = VMEM((144, 128), F32)
LOW_FACES = VMEM((48, 128), F32)


def in_vmem(value):
    return pltpu.with_memory_space_constraint(value, VMEM)


def in_hbm(value):
    return pltpu.with_memory_space_constraint(value, pltpu.HBM)


def call(body, outs, args, scratch=(), smem=(), smem_outs=(), far=False, far_out=False):
    spec = pl.BlockSpec(memory_space=VMEM)
    source = pl.BlockSpec(memory_space=pl.ANY) if far else spec
    target = pl.BlockSpec(memory_space=pl.ANY) if far_out else spec
    scalar = pl.BlockSpec(memory_space=pltpu.SMEM)
    return pl.pallas_call(
        body,
        out_shape=list(outs),
        in_specs=[scalar if at in smem else source for at in range(len(args))],
        out_specs=[scalar if at in smem_outs else target for at in range(len(outs))],
        scratch_shapes=list(scratch),
        compiler_params=pltpu.CompilerParams(vmem_limit_bytes=6 * 1024 * 1024),
    )(*args)


def odd_swap(value):
    count = lax.axis_size("dom")
    route = []
    for at in range(1, count - 1, 2):
        route += [(at, at + 1), (at + 1, at)]
    return lax.ppermute(value, "dom", route)


def even_swap(value):
    return in_vmem(lax.ppermute(value, "dom", [(at, at ^ 1) for at in range(lax.axis_size("dom"))]))


def cycle(rhs, stiffness, vol_jac, face_jac, block_inv, face_owner, face_elem, face_side, face_turn):
    me = lax.axis_index("dom").astype(jnp.int32).reshape(1)
    rhs_state = rhs.reshape(4, 12, 4, 128).transpose(1, 2, 0, 3).reshape(24, 8, 128)
    inverse = block_inv.reshape(4, 12, 12, 4, 128).transpose(1, 2, 3, 0, 4).reshape(288, 8, 128)
    vj = vol_jac.transpose(1, 0, 2).reshape(6, 8, 12)
    fj = face_jac.transpose(1, 2, 0, 3).reshape(36, 8, 12)
    trace = jnp.asarray(np.concatenate([trace_matrix(), low_trace_matrix()], 1), BF16)
    lift = jnp.asarray(lift_matrix(), BF16)
    numbers = (face_owner, face_elem, face_side, face_turn)
    integers = pltpu.SMEM((24,), jnp.int32)
    indices = VMEM((6, 8, 128), jnp.int32)
    signs = VMEM((3, 8, 128), F32)
    u, split, faces, message, inverse, rhs_state, trace = call(
        first_body,
        (
            STATE,
            SPLIT,
            FACES,
            VMEM((MESSAGE_ROWS, 128), F32),
            VMEM((288, 8, 128), F32),
            STATE,
            VMEM(trace.shape, BF16),
        ),
        (me, *(in_hbm(load) for load in (*numbers, fj, inverse, rhs_state, trace))),
        (VMEM((36, 8, 12), F32), *(VMEM((4, 6), jnp.int32) for _ in range(4)), pltpu.SemaphoreType.DMA((8,))),
        smem=(0,),
        far=True,
    )
    far_message = in_vmem(odd_swap(message))
    even = even_swap(faces)
    loads = (*numbers, vj, fj, stiffness, lift)
    start, idx, sign, low_start, low_idx, near, far, low_plain, short_start, short_idx, vjc, fjc, khi, klo, lift = call(
        prepare_body,
        (
            integers,
            indices,
            signs,
            integers,
            indices,
            signs,
            signs,
            integers,
            integers,
            indices,
            VMEM((144, 8, 128), F32),
            VMEM((216, 8, 128), F32),
            VMEM((512, 512), BF16),
            VMEM((512, 512), BF16),
            VMEM((384, 512), BF16),
        ),
        (me, *(in_hbm(load) for load in loads)),
        (
            *(pltpu.SMEM((4, 6), jnp.int32) for _ in range(4)),
            VMEM((6, 8, 12), F32),
            VMEM((36, 8, 12), F32),
            VMEM((512, 512), F32),
            pltpu.SemaphoreType.DMA((8,)),
        ),
        smem=(0,),
        smem_outs=(0, 3, 7, 8),
        far=True,
    )
    volume = (vjc, fjc, khi, klo, lift)
    picks = (FACES, FACES, VMEM((96, 384), BF16))
    pool = (VMEM((432, 128), F32), *picks)

    fine_two, split, faces, sent = call(
        fine_low_body,
        (STATE, SPLIT, FACES, LOW_FACES),
        (inverse, trace, u, rhs_state, split, faces, faces, even, far_message, start, idx, sign, *volume),
        pool,
        smem=(9,),
    )
    even = even_swap(sent)
    (payload,) = call(
        local_low_body,
        (FACES,),
        (fine_two, rhs_state, split, faces, sent, even, low_start, low_idx, near, *volume),
        pool,
        smem=(6,),
    )
    far_payload = in_vmem(odd_swap(payload))
    ghost_start, ghost_idx, ghost_sign, ghost_fjc, ghost_inverse, ask, ask_idx = call(
        ghost_prepare_body,
        (
            integers,
            indices,
            signs,
            VMEM((216, 8, 128), F32),
            VMEM((144, 8, 128), F32),
            pltpu.SMEM((32,), jnp.int32),
            VMEM((2, 8, 128), jnp.int32),
        ),
        (me, far_message),
        (
            pltpu.SMEM((24,), jnp.int32),
            VMEM((6, 8, 128), jnp.int32),
            pltpu.SMEM((32,), jnp.int32),
            pltpu.SMEM((16, 128), F32),
            pltpu.SemaphoreType.DMA((1,)),
        ),
        smem=(0,),
        smem_outs=(0, 5),
    )
    low_rhs, coarse, split, faces, sent = call(
        own_low_body,
        (STATE, STATE, SPLIT, FACES, LOW_FACES),
        (inverse, trace, payload, far_payload, low_plain, low_idx, far, fjc, lift),
        picks,
        smem=(4,),
    )
    even = even_swap(sent)
    (odd,) = call(
        ghost_low_body,
        (LOW_FACES,),
        (ghost_inverse, trace, payload, far_payload, ghost_start, ghost_idx, ghost_sign, ghost_fjc, lift),
        (*picks, SPLIT, FACES),
        smem=(4,),
    )
    tables = (short_start, short_idx, sign, *volume)
    u, split, faces, short = call(
        coarse_body,
        (STATE, SPLIT, FACES, LOW_FACES),
        (inverse, trace, fine_two, coarse, low_rhs, split, faces, sent, even, odd, low_start, low_idx, sign, *volume, ask, ask_idx),
        pool,
        smem=(10, 18),
    )
    odd = in_vmem(odd_swap(short))
    even = even_swap(faces)
    u, split, faces, short = call(
        fine_body,
        (STATE, SPLIT, FACES, LOW_FACES),
        (inverse, trace, u, rhs_state, split, faces, faces, even, odd, *tables, ask, ask_idx),
        pool,
        smem=(9, 17),
    )
    odd = in_vmem(odd_swap(short))
    even = even_swap(faces)
    (u,) = call(
        last_body,
        (jax.ShapeDtypeStruct((24, 8, 128), F32),),
        (inverse, u, rhs_state, split, faces, faces, even, odd, *tables),
        (*pool, STATE, pltpu.SemaphoreType.DMA((3,))),
        smem=(8,),
        far_out=True,
    )
    return u.reshape(12, 4, 4, 128).transpose(2, 0, 1, 3).reshape(4, 12, 512)


def solution(mesh):
    dom = P("dom")
    return jax.shard_map(
        cycle,
        mesh=mesh,
        in_specs=(dom, P(), dom, dom, dom, dom, dom, dom, dom),
        out_specs=dom,
        check_vma=False,
    )
```
